32 devices in a mesh: row: 4 (over x, core), col: 8 (over z, y).
Axes of the slice: x: 2, y: 2, z: 4, core: 2. Of those that a mesh axis runs over, the one named last changes fastest.
Arguments:
- resistance: float32 [4096, 8192], P('row', 'col'), may hold values from 1 to 100
- source_mask: int32 [4096, 8192], P('row', 'col'), may hold values 0 or 1
- target_mask: int32 [4096, 8192], P('row', 'col'), may hold values 0 or 1
- centers: int32 [512, 2], P(('row', 'col')), may hold values from 0 to 8191, as said below
- live_counts: int32 [32], P(('row', 'col')), may hold values from 1 to 16, 128 in all
Outputs:
- current_map: float32 [4096, 8192], P('row', 'col')
The draws below stay inside these ranges and needn't reach their ends.
Inputs may be any that keep to these rules, and one draw needn't show every extreme that they name: `centers`: the center of slot s lies inside the block of raster cells held by device s // 16 (numbered along row+col, row slowest). Slots 0 to live_counts[d] - 1 of device d are live; some device has all 16 slots live.
All inputs are finite; a program needn't handle non-finite values. No bound on the sum of `source_mask` or of `target_mask` on one device may be relied on, other than what follows from the above.
Results may differ from the reference program's by a relative error of at most 0.0003.
Values sent between devices are 32-bit elements; how exact they have to be, the bound alone decides.
A program may use at most 128 MiB of HBM per device.

```python
import math
import jax
import jax.numpy as jnp
import numpy as np
from jax import lax

TILE_R = 1024
TILE_C = 1024
RAD = 64
ITERS = 24
WCAP = 16
H = 4096
W = 8192
NWIN = 512
DEVICES = 32


def draw_centers(key, part):
    device = jnp.arange(NWIN, dtype=jnp.int32) // WCAP
    col_devices = W // TILE_C
    device_row = device // col_devices
    device_col = device % col_devices
    key_rows = jax.random.fold_in(key, 11)
    key_cols = jax.random.fold_in(key, 23)
    rows_in = jax.random.randint(key_rows, (NWIN,), 0, TILE_R, dtype=jnp.int32)
    cols_in = jax.random.randint(key_cols, (NWIN,), 0, TILE_C, dtype=jnp.int32)
    return jnp.stack([device_row * TILE_R + rows_in, device_col * TILE_C + cols_in], axis=1)


def touch_ends(result, key, smallest, high):
    longest = result.shape.index(max(result.shape))
    spots = []
    for shift in (0, 1):
        where = [jax.random.randint(jax.random.fold_in(key, axis), (), 0, length) for axis, length in enumerate(result.shape)]
        where[longest] = (where[longest] + shift) % result.shape[longest]
        spots.append(tuple(where))
    return result.at[spots[0]].set(smallest).at[spots[1]].set(high)


def steps_of(stream_key, shape, cuts, least, largest):
    gain = 1.0
    for axis_at, parts in cuts:
        heights = jax.random.uniform(jax.random.fold_in(jax.random.fold_in(stream_key, 6), axis_at), (parts,), jnp.float32, least / len(cuts), largest / len(cuts))
        gain = gain * jnp.repeat(jnp.exp(heights), shape[axis_at] // parts).reshape((-1,) + (1,) * (len(shape) - 1 - axis_at))
    return gain


def length_profile(amount, total, limit, lean):
    weights = [(1 << 20) // math.isqrt(standing ** lean) + 1 for standing in range(2, amount + 1)]
    surplus, given = total - limit - (amount - 1), [1] * (amount - 1)
    while surplus > 0:
        free = [i for i in range(amount - 1) if given[i] < limit]
        pool, left = sum([weights[i] for i in free]), surplus
        for i in free:
            extra = min(limit - given[i], max(1, left * weights[i] // pool), surplus)
            given[i] = given[i] + extra
            surplus = surplus - extra
    return np.array([limit] + given)


def uneven_parts(own_key, number_of, total, limit, skew):
    if number_of == 2:
        one = jax.random.randint(own_key, (), max(1, total - limit), min(limit, total - 1) + 1)
        return jnp.stack([one, total - one])
    tallies = jnp.asarray(length_profile(number_of, total, limit, skew), jnp.int32)
    pairs = (number_of - 1) // 2
    donor, receiver = tallies[1:1 + 2 * pairs:2], tallies[2:2 + 2 * pairs:2]
    margin = jnp.minimum(donor - 1, limit - receiver)
    passed = jax.random.randint(jax.random.fold_in(own_key, 1), (pairs,), 0, 1 << 20) % (margin + 1)
    tallies = tallies.at[1:1 + 2 * pairs:2].set(donor - passed).at[2:2 + 2 * pairs:2].set(receiver + passed)
    return tallies[jax.random.permutation(jax.random.fold_in(own_key, 2), number_of)]


def setup_inputs(seed: int = 0) -> dict:
    key_list = jax.random.split(jax.random.key(seed), 6)
    return {
        "resistance": jnp.clip(jnp.exp(math.log(100.0) - 4.6051702 * jax.random.uniform(key_list[0], (H, W), jnp.float32) ** steps_of(key_list[0], (H, W), ((0, 4), (1, 8)), -0.2, 0.2)), 1.0, 100.0),
        "source_mask": touch_ends((jax.random.randint(key_list[1], (H, W), 0, 2) < 1).astype(jnp.int32), jax.random.fold_in(key_list[1], 1), 0, 1),
        "target_mask": touch_ends((jax.random.randint(key_list[2], (H, W), 0, 8) < 1).astype(jnp.int32), jax.random.fold_in(key_list[2], 1), 0, 1),
        "centers": draw_centers(jax.random.fold_in(key_list[5], 71), 0),
        "live_counts": uneven_parts(key_list[4], DEVICES, DEVICES * WCAP // 4, WCAP, 2).astype(jnp.int32),
    }


LEAKAGE = 0.02


def edge_terms(resist):
    inside = (resist > 0.0).astype(jnp.float32)
    safe_res = jnp.where(resist > 0.0, resist, 1.0)
    side_len = resist.shape[-1]
    row_pos = lax.broadcasted_iota(jnp.int32, (side_len, side_len), 0)
    col_pos = lax.broadcasted_iota(jnp.int32, (side_len, side_len), 1)
    not_last_row = (row_pos < side_len - 1).astype(jnp.float32)
    not_last_col = (col_pos < side_len - 1).astype(jnp.float32)
    vertical = not_last_row * inside * jnp.roll(inside, -1, 1) * 2.0 / (safe_res + jnp.roll(safe_res, -1, 1))
    horizontal = not_last_col * inside * jnp.roll(inside, -1, 2) * 2.0 / (safe_res + jnp.roll(safe_res, -1, 2))
    return vertical, horizontal


def window_sum(values):
    return jnp.sum(values, axis=(1, 2), keepdims=True)


def solve_windows(resist, signed):
    vertical, horizontal = edge_terms(resist)
    side_len = resist.shape[-1]
    row_pos = lax.broadcasted_iota(jnp.int32, (side_len, side_len), 0)
    col_pos = lax.broadcasted_iota(jnp.int32, (side_len, side_len), 1)
    center = ((row_pos == RAD) & (col_pos == RAD)).astype(jnp.float32)
    inject = jnp.maximum(signed, 0.0) + center
    ground = jnp.maximum(-signed, 0.0)
    diagonal = vertical + jnp.roll(vertical, 1, 1) + horizontal + jnp.roll(horizontal, 1, 2) + ground + LEAKAGE

    def operate(field):
        beside = vertical * jnp.roll(field, -1, 1) + jnp.roll(vertical * field, 1, 1)
        beside = beside + horizontal * jnp.roll(field, -1, 2) + jnp.roll(horizontal * field, 1, 2)
        return diagonal * field - beside

    voltage = jnp.zeros_like(inject)
    residual = inject
    scaled = residual / diagonal
    direction = scaled
    product_now = window_sum(residual * scaled)
    for repeat in range(ITERS):
        applied = operate(direction)
        step_size = product_now / window_sum(direction * applied)
        voltage = voltage + step_size * direction
        residual = residual - step_size * applied
        scaled = residual / diagonal
        product_next = window_sum(residual * scaled)
        direction = scaled + (product_next / product_now) * direction
        product_now = product_next
    flow_down = vertical * jnp.abs(voltage - jnp.roll(voltage, -1, 1))
    flow_right = horizontal * jnp.abs(voltage - jnp.roll(voltage, -1, 2))
    total_flow = flow_down + jnp.roll(flow_down, 1, 1) + flow_right + jnp.roll(flow_right, 1, 2)
    return 0.5 * (total_flow + inject + ground * jnp.abs(voltage))


def reference(resistance, source_mask, target_mask, centers, live_counts):
    conduct = 1.0 / resistance
    sources = source_mask.astype(jnp.float32)
    targets = target_mask.astype(jnp.float32)
    signed = sources * conduct - targets * (1.0 - sources) * conduct
    side_len = 2 * RAD
    padded_res = jnp.pad(resistance, RAD)
    padded_sign = jnp.pad(signed, RAD)
    accumulated = jnp.zeros((H + 2 * RAD, W + 2 * RAD), jnp.float32)

    def add_window(total_map, slot_index):
        top_row = centers[slot_index, 0].astype(jnp.int32)
        left_col = centers[slot_index, 1].astype(jnp.int32)
        is_live = (slot_index % WCAP < live_counts[slot_index // WCAP]).astype(jnp.float32)
        win_res = lax.dynamic_slice(padded_res, (top_row, left_col), (side_len, side_len))[None]
        win_sign = lax.dynamic_slice(padded_sign, (top_row, left_col), (side_len, side_len))[None]
        current = solve_windows(win_res, win_sign)[0] * is_live
        previous = lax.dynamic_slice(total_map, (top_row, left_col), (side_len, side_len))
        return lax.dynamic_update_slice(total_map, previous + current, (top_row, left_col)), None

    accumulated, unused = lax.scan(add_window, accumulated, jnp.arange(NWIN, dtype=jnp.int32))
    return accumulated[RAD:RAD + H, RAD:RAD + W]
```

```python
import functools

import jax
import jax.numpy as jnp
from jax import lax
from jax.experimental import pallas as pl
from jax.experimental.pallas import tpu as pltpu
from jax.sharding import PartitionSpec as P

RAD = 64
SIDE = 2 * RAD
ITERS = 24
LEAKAGE = 0.02
FAR = 1e37
QUADS = 2
GROUP = 4 * QUADS
LANES = 128
TALL = SIDE + 8
WIDE = 2 * LANES
SHIFTS = ((0, -1), (0, 1), (-1, 0), (1, 0), (-1, -1), (-1, 1), (1, -1), (1, 1))


def roll(value, shift, axis):
    return pltpu.roll(value, shift % value.shape[axis], axis)


def lane_ids(shape):
    return lax.broadcasted_iota(jnp.int32, shape, 1)


def to_low(packed):
    return packed, roll(packed, RAD, 1)


def to_high(packed):
    return roll(packed, RAD, 1), packed


def pack_low(tile):
    half = tile.shape[0] // 2
    first, second = tile[:half], tile[half:]
    return jnp.where(lane_ids(first.shape) < RAD, first, roll(second, RAD, 1))


def pack_high(tile):
    half = tile.shape[0] // 2
    first, second = tile[:half], tile[half:]
    return jnp.where(lane_ids(first.shape) < RAD, roll(first, RAD, 1), second)


def neighbours():
    row, col = lax.axis_index("row"), lax.axis_index("col")
    rows, cols = lax.axis_size("row"), lax.axis_size("col")
    found = {}
    for (dr, dc) in SHIFTS:
        r, c = row + dr, col + dc
        found[(dr, dc)] = ((r >= 0) & (r < rows) & (c >= 0) & (c < cols), (r, c))
    return found


def greet(found):
    barrier = pltpu.get_barrier_semaphore()
    for at in SHIFTS:
        exists, device = found[at]

        @pl.when(exists)
        def _():
            pl.semaphore_signal(barrier, inc=1, device_id=device, device_id_type=pl.DeviceIdType.MESH)


def all_greeted(found):
    count = sum(found[at][0].astype(jnp.int32) for at in SHIFTS)
    pl.semaphore_wait(pltpu.get_barrier_semaphore(), count)


def transfers(found, pieces, halos, send_sems, recv_sems):
    made = []
    for k, at in enumerate(SHIFTS):
        exists, device = found[at]
        back = (-at[0], -at[1])
        made.append((exists, pltpu.make_async_remote_copy(
            src_ref=pieces[at],
            dst_ref=halos[back],
            send_sem=send_sems.at[k],
            recv_sem=recv_sems.at[SHIFTS.index(back)],
            device_id=device,
            device_id_type=pl.DeviceIdType.MESH,
        )))
    return made


def landings(found, pieces, halos, send_sems, recv_sems):
    made = []
    for k, at in enumerate(SHIFTS):
        exists, device = found[at]
        made.append((exists, pltpu.make_async_remote_copy(
            src_ref=pieces[at],
            dst_ref=halos[at],
            send_sem=send_sems.at[k],
            recv_sem=recv_sems.at[k],
            device_id=device,
            device_id_type=pl.DeviceIdType.MESH,
        )))
    return made


def start_all(copies):
    for exists, copy in copies:
        pl.when(exists)(copy.start)


def finish_all(copies, arrivals):
    for exists, copy in copies:
        pl.when(exists)(copy.wait_send)
    for exists, copy in arrivals:
        pl.when(exists)(copy.wait_recv)


def corner_of(centers, slot, rows, cols):
    return lax.rem(centers[slot, 0], rows) - RAD, lax.rem(centers[slot, 1], cols) - RAD


def is_inner(top, left, rows, cols):
    return (top >= 0) & (top <= rows - SIDE) & (left >= 0) & (left <= cols - SIDE)


def clamped(top, left, rows, cols):
    row = jnp.clip((top + RAD) // 8 * 8 - RAD, 0, rows - TALL)
    col = jnp.clip((left + LANES) // LANES * LANES - LANES, 0, cols - WIDE)
    return pl.multiple_of(row, 8), pl.multiple_of(col, LANES)


def total(values):
    return jnp.sum(jnp.sum(values, axis=0, keepdims=True), axis=1, keepdims=True)


def cut_rows(value, skip):
    return pltpu.roll(value, lax.rem(TALL - skip, TALL), 0)[:SIDE]


def add_window(acc, current, top, left):
    col = pl.multiple_of((left + LANES) // LANES * LANES, LANES)
    shift = left + LANES - col
    wide = jnp.concatenate([current, jnp.zeros_like(current)], axis=1)
    wide = pltpu.roll(wide, shift, 1)
    wide = jnp.concatenate([wide, jnp.zeros((8, WIDE), jnp.float32)], axis=0)
    wide = pltpu.roll(wide, lax.rem(top + RAD, 8), 0)
    rows = pl.ds(pl.multiple_of((top + RAD) // 8 * 8, 8), TALL)
    acc[rows, pl.ds(col, WIDE)] = acc[rows, pl.ds(col, WIDE)] + wide


PLANES = 4
CHUNK = 64
SEGMENTS = SIDE // PLANES
EIGHTS = tuple(slice(8 * k, 8 * k + 8) for k in range(SIDE // 8))


def lanes_of(shape):
    return lax.broadcasted_iota(jnp.int32, shape, 1)


def interleave(shape, transposed):
    row, col = (lax.broadcasted_iota(jnp.int32, shape, axis) for axis in (0, 1))
    if transposed:
        row, col = col, row
    window, place = row // SIDE, row % SIDE
    return (col == (place % PLANES) * SIDE + window * SEGMENTS + place // PLANES).astype(jnp.bfloat16)


def halves(value):
    high = value.astype(jnp.bfloat16)
    return high, (value - high.astype(jnp.float32)).astype(jnp.bfloat16)


def mixed(parts, table):
    found = jnp.dot(jnp.concatenate(parts, axis=0), table[...], preferred_element_type=jnp.float32)
    size = parts[0].shape[0]
    return [found[size * n:size * n + size] for n in range(len(parts))]


def quad_state():
    f32 = jnp.float32
    planes = pltpu.VMEM((PLANES, SIDE, SIDE), f32)
    padded = pltpu.VMEM((PLANES, SIDE + 16, SIDE), f32)
    tile = pltpu.VMEM((SIDE, SIDE), f32)
    table = pltpu.VMEM((ITERS, 8, SIDE), f32)
    return (
        [padded, padded, pltpu.VMEM((ITERS, PLANES, SIDE, SIDE), f32), planes]
        + [padded, planes, tile]
        + [tile, tile]
        + [padded, planes, planes, padded, padded, planes]
        + [table, table]
    )


def solver_state():
    wide = PLANES * SIDE
    return quad_state() * QUADS + [pltpu.VMEM((2, wide, wide), jnp.bfloat16)]


def quad_parts(state):
    even, odd, hist, t_s, vert, hori, hori_in, edge_r, edge_l, isd_s, inj_s, gnd_s, v_s, res_s, h_s, tail_s, link_s = state
    f32 = jnp.float32
    mid = tuple(slice(8 + 8 * k, 16 + 8 * k) for k in range(SIDE // 8))
    low = tuple(slice(9 + 8 * k, 17 + 8 * k) for k in range(SIDE // 8))
    upp = tuple(slice(7 + 8 * k, 15 + 8 * k) for k in range(SIDE // 8))
    blocks = range(SIDE // 8)
    lane = lanes_of((8, SIDE))
    row8 = lax.broadcasted_iota(jnp.int32, (8, SIDE), 0)

    def clear():
        zero = jnp.zeros((8, SIDE), f32)
        for pad in (even, odd, vert, isd_s, v_s, res_s):
            for p in range(PLANES):
                pad[p, 0:8, :] = zero
                pad[p, 8 + SIDE:16 + SIDE, :] = zero

    def refresh_edges(cur):
        for k in blocks:
            edge_r[EIGHTS[k], :] = roll(cur[0, mid[k], :], -1, 1)
            edge_l[EIGHTS[k], :] = roll(cur[PLANES - 1, mid[k], :], 1, 1)

    def operate(cur):
        gammas, deltas = [None] * PLANES, [None] * PLANES
        for k in blocks:
            here = [cur[p, mid[k], :] for p in range(PLANES)]
            out = [hori[p, EIGHTS[k], :] for p in range(PLANES)]
            for p in (1, 2, 0, 3):
                right = here[p + 1] if p < PLANES - 1 else edge_r[EIGHTS[k], :]
                left = here[p - 1] if p else edge_l[EIGHTS[k], :]
                back = out[p - 1] if p else hori_in[EIGHTS[k], :]
                beside = vert[p, mid[k], :] * cur[p, low[k], :] + vert[p, upp[k], :] * cur[p, upp[k], :]
                beside = beside + (out[p] * right + back * left)
                t_s[p, EIGHTS[k], :] = beside
                one, two = here[p] * here[p], here[p] * beside
                gammas[p] = one if k == 0 else gammas[p] + one
                deltas[p] = two if k == 0 else deltas[p] + two
        return (gammas[0] + gammas[1]) + (gammas[2] + gammas[3]), (deltas[0] + deltas[1]) + (deltas[2] + deltas[3])

    def down_sum(part):
        for shift in (4, 2, 1):
            part = part + roll(part, shift, 0)
        return part

    def total_of(sums):
        mine = lane // SEGMENTS == row8 % PLANES
        first = row8 < PLANES
        both = jnp.where(first, down_sum(sums[0]), down_sum(sums[1]))
        both = jnp.where(mine, jnp.sum(jnp.where(mine, both, 0.0), axis=1, keepdims=True), 0.0)
        return down_sum(jnp.where(first, both, 0.0)), down_sum(jnp.where(first, 0.0, both))

    def prepare(load, table):
        for r in range(0, SIDE, CHUNK):
            cut = slice(r, r + CHUNK)
            loaded = [load(w, cut) for w in range(PLANES)]
            res = jnp.concatenate([pair[0] for pair in loaded], axis=1)
            mark = jnp.concatenate([pair[1] for pair in loaded], axis=1)
            high, low_part, mark = mixed([*halves(res), mark.astype(jnp.bfloat16)], table)
            res = high + low_part
            signed = mark / res
            for p in range(PLANES):
                span = slice(SIDE * p, SIDE * p + SIDE)
                res_s[p, 8 + r:8 + r + CHUNK, :] = res[:, span]
                inject = jnp.maximum(signed[:, span], 0.0)
                if p == 0 and r <= RAD < r + CHUNK:
                    at = lax.broadcasted_iota(jnp.int32, (CHUNK, SIDE), 0) == RAD - r
                    spot = lanes_of((CHUNK, SIDE)) % SEGMENTS == RAD // PLANES
                    inject = inject + (at & spot).astype(f32)
                inj_s[p, cut, :] = inject
                gnd_s[p, cut, :] = jnp.maximum(-signed[:, span], 0.0)
        ends = lane % SEGMENTS == SEGMENTS - 1
        bottom = row8 == 7
        for k in blocks:
            for p in range(PLANES):
                here = res_s[p, mid[k], :]
                under = res_s[p, low[k], :]
                if k == len(EIGHTS) - 1:
                    vertical = jnp.where(bottom, 0.0, 2.0 / (here + jnp.where(bottom, FAR, under)))
                else:
                    vertical = 2.0 / (here + under)
                v_s[p, mid[k], :] = vertical
                if p < PLANES - 1:
                    h_s[p, EIGHTS[k], :] = 2.0 / (here + res_s[p + 1, mid[k], :])
                else:
                    horizontal = jnp.where(ends, 0.0, 2.0 / (here + roll(res_s[0, mid[k], :], -1, 1)))
                    h_s[p, EIGHTS[k], :] = horizontal
                    edge_l[EIGHTS[k], :] = roll(horizontal, 1, 1)
        for k in blocks:
            for p in range(PLANES):
                before = h_s[p - 1, EIGHTS[k], :] if p else edge_l[EIGHTS[k], :]
                diagonal = v_s[p, mid[k], :] + v_s[p, upp[k], :] + (h_s[p, EIGHTS[k], :] + before)
                isd_s[p, mid[k], :] = 1.0 / jnp.sqrt(diagonal + gnd_s[p, EIGHTS[k], :] + LEAKAGE)
        for k in blocks:
            for p in range(PLANES):
                isd = isd_s[p, mid[k], :]
                vert[p, mid[k], :] = v_s[p, mid[k], :] * isd * isd_s[p, low[k], :]
                if p < PLANES - 1:
                    hori[p, EIGHTS[k], :] = h_s[p, EIGHTS[k], :] * isd * isd_s[p + 1, mid[k], :]
                else:
                    scaled = h_s[p, EIGHTS[k], :] * isd * roll(isd_s[0, mid[k], :], -1, 1)
                    hori[p, EIGHTS[k], :] = scaled
                    hori_in[EIGHTS[k], :] = roll(scaled, 1, 1)
                first = inj_s[p, EIGHTS[k], :] * isd
                even[p, mid[k], :] = first
                hist[0, p, EIGHTS[k], :] = first
        refresh_edges(even)
        return operate(even)

    def settle(j, sums, gamma_inv_before, pivot_inv, weight):
        gamma, delta = sums
        gamma_inv = 1.0 / gamma
        mean = delta * gamma_inv
        ratio = gamma * gamma_inv_before
        link = ratio * pivot_inv
        pivot_inv = 1.0 / (1.0 - mean - link)
        weight = weight * pivot_inv
        tail_s[j] = weight
        link_s[j] = link
        return mean, ratio, gamma_inv, pivot_inv, weight

    def update(j, way, mean, ratio):
        cur, new = (odd, even) if way else (even, odd)
        for p in (0, 3, 1, 2):
            for k in blocks:
                fresh = t_s[p, EIGHTS[k], :] - mean * cur[p, mid[k], :]
                if ratio is not None:
                    fresh = fresh - ratio * new[p, mid[k], :]
                new[p, mid[k], :] = fresh
                hist[j + 1, p, EIGHTS[k], :] = fresh
                if p == 0:
                    edge_r[EIGHTS[k], :] = roll(fresh, -1, 1)
                if p == PLANES - 1:
                    edge_l[EIGHTS[k], :] = roll(fresh, 1, 1)
        return operate(new)

    def coefficients():
        factor = tail_s[ITERS - 1]
        for j in reversed(range(1, ITERS)):
            ahead = tail_s[j - 1] + link_s[j] * factor
            tail_s[j] = factor
            factor = ahead
        tail_s[0] = factor

    def voltages():
        def one(p, _):
            for half in range(2):
                found = [None] * 8
                for j in range(ITERS):
                    factor = tail_s[j]
                    for i in range(8):
                        term = factor * hist[j, p, EIGHTS[8 * half + i], :]
                        found[i] = term if found[i] is None else found[i] + term
                for i in range(8):
                    even[p, mid[8 * half + i], :] = found[i] * isd_s[p, mid[8 * half + i], :]
            return 0

        lax.fori_loop(0, PLANES, one, 0)

    def finish(put, table):
        cur = even
        for k in blocks:
            edge_r[EIGHTS[k], :] = roll(cur[0, mid[k], :], -1, 1)
        for k in blocks:
            for p in range(PLANES):
                volts = cur[p, mid[k], :]
                res_s[p, mid[k], :] = v_s[p, mid[k], :] * jnp.abs(volts - cur[p, low[k], :])
                right = cur[p + 1, mid[k], :] if p < PLANES - 1 else edge_r[EIGHTS[k], :]
                flow = h_s[p, EIGHTS[k], :] * jnp.abs(volts - right)
                t_s[p, EIGHTS[k], :] = flow
                if p == PLANES - 1:
                    edge_l[EIGHTS[k], :] = roll(flow, 1, 1)

        for r in range(0, SIDE, CHUNK):
            cut = slice(r, r + CHUNK)
            pieces = []
            for p in range(PLANES):
                flow = res_s[p, 8 + r:8 + r + CHUNK, :] + res_s[p, 7 + r:7 + r + CHUNK, :] + t_s[p, cut, :]
                flow = flow + (t_s[p - 1, cut, :] if p else edge_l[cut, :])
                pieces.append(0.5 * (flow + inj_s[p, cut, :] + gnd_s[p, cut, :] * jnp.abs(cur[p, 8 + r:8 + r + CHUNK, :])))
            high, low_part = mixed(halves(jnp.concatenate(pieces, axis=1)), table)
            for w in range(PLANES):
                span = slice(SIDE * w, SIDE * w + SIDE)
                put(w, cut, high[:, span] + low_part[:, span])

    return clear, prepare, total_of, operate, settle, update, coefficients, voltages, finish


def solver_parts(state):
    table = state[-1]
    size = (len(state) - 1) // QUADS
    quads = [quad_parts(state[size * q:size * q + size]) for q in range(QUADS)]

    def clear():
        for quad in quads:
            quad[0]()
        for way in range(2):
            table[way] = interleave(table.shape[1:], way == 1)

    def solve(load, store):
        one = jnp.ones((8, SIDE), jnp.float32)
        carry = []
        for q, (_, prepare, total_of, *_) in enumerate(quads):
            sums = prepare(lambda w, cut, q=q: load(PLANES * q + w, cut), table.at[0])
            carry.append((sums if q else total_of(sums), 0.0 * one, 0.0 * one, one))

        def step(j, way, carry, first=False):
            after = []
            for q, (_, _, total_of, operate, settle, update, *_) in enumerate(quads):
                sums, *rest = carry[q]
                if q:
                    sums = total_of(sums)
                mean, ratio, *rest = settle(j, sums, *rest)
                sums = update(j, way, mean, None if first else ratio)
                after.append((sums if q else total_of(sums), *rest))
            return after

        def steps(i, carry):
            return tuple(step(2 * i + 2, 0, step(2 * i + 1, 1, carry)))

        carry = tuple(step(0, 0, carry, True))
        carry = lax.fori_loop(0, (ITERS - 2) // 2, steps, carry)
        for q, (_, _, total_of, _, settle, _, coefficients, *_) in enumerate(quads):
            settle(ITERS - 1, total_of(carry[q][0]) if q else carry[q][0], *carry[q][1:])
            coefficients()
        for q, (*_, voltages, finish) in enumerate(quads):
            voltages()
            finish(lambda w, cut, tile, q=q: store(PLANES * q + w, cut, tile), table.at[1])

    return clear, solve


def spans_of(rows, cols):
    return {
        -1: (slice(0, RAD), slice(0, LANES)),
        0: (slice(RAD, RAD + rows), slice(LANES, LANES + cols)),
        1: (slice(RAD + rows, SIDE + rows), slice(LANES + cols, WIDE + cols)),
    }


def turn_own(res, source, target, skip, turn):
    source, target = source.astype(jnp.float32), target.astype(jnp.float32)
    mark = source - target * (1.0 - source)
    turn = lax.rem(WIDE + turn, WIDE)
    res = cut_rows(pltpu.roll(res, turn, 1)[:, :SIDE], skip)
    mark = cut_rows(pltpu.roll(mark, turn, 1)[:, :SIDE], skip)
    return res, mark


def cut_kernel(rows, cols, centers, live, *refs):
    raw, out, bufs, sems = refs[:3], refs[3], refs[4:7], refs[7]

    def place(slot):
        top, left = corner_of(centers, slot, rows, cols)
        return top, left, *clamped(top, left, rows, cols)

    def copies(slot):
        _, _, row, col = place(slot)
        return [
            pltpu.make_async_copy(src.at[pl.ds(row, TALL), pl.ds(col, WIDE)], dst.at[slot], sems.at[k, slot])
            for k, (src, dst) in enumerate(zip(raw, bufs))
        ]

    def begin(slot, _):
        for copy in copies(slot):
            copy.start()
        return 0

    def cut(slot, _):
        for copy in copies(slot):
            copy.wait()
        top, left, row, col = place(slot)
        res, mark = turn_own(*(buf[slot] for buf in bufs), top - row, col - left)
        out[0, slot] = res
        out[1, slot] = mark
        return 0

    def blank(slot, _):
        out[0, slot] = jnp.ones((SIDE, SIDE), jnp.float32)
        out[1, slot] = jnp.zeros((SIDE, SIDE), jnp.float32)
        return 0

    lax.fori_loop(0, live[0], begin, 0)
    lax.fori_loop(live[0], out.shape[1], blank, 0)
    lax.fori_loop(0, live[0], cut, 0)


def inner_kernel(rows, cols, windows, *refs):
    raw = refs[:3]
    cur, outs = refs[3], dict(zip(SHIFTS, refs[4:12]))
    pieces, halos = dict(zip(SHIFTS, refs[12:20])), dict(zip(SHIFTS, refs[20:28]))
    frames = [refs[28 + 3 * k:31 + 3 * k] for k in range(4)]
    sems, send_sems, recv_sems = refs[40:43]
    clear, solve = solver_parts(refs[43:])
    slots = windows.shape[1]
    found = neighbours()
    clear()

    everything = pl.ds(0, rows)
    places = (
        (everything, pl.ds(0, LANES)),
        (everything, pl.ds(cols - LANES, LANES)),
        (pl.ds(0, RAD), pl.ds(0, cols)),
        (pl.ds(rows - RAD, RAD), pl.ds(0, cols)),
    )
    frame_copies = [
        [pltpu.make_async_copy(raw[k].at[places[f]], frames[f][k], sems.at[f, k]) for k in range(3)]
        for f in range(4)
    ]
    for copy in sum(frame_copies, []):
        copy.start()
    for at in SHIFTS:
        halos[at][...] = jnp.zeros_like(halos[at])
    greet(found)

    def strengths(frame, cut=slice(None)):
        res, source, target = (ref[cut] for ref in frame)
        source, target = source.astype(jnp.float32), target.astype(jnp.float32)
        return res, source - target * (1.0 - source)

    for f, at in enumerate(((0, -1), (0, 1), (-1, 0), (1, 0))):
        for copy in frame_copies[f]:
            copy.wait()
        for k, value in enumerate(strengths(frames[f])):
            if at[1] == 0:
                pieces[at][k] = value
            else:
                squeeze = pack_low if at[1] < 0 else pack_high
                pieces[at][k] = squeeze(value)
                pieces[(-1, at[1])][k] = squeeze(value[:RAD])
                pieces[(1, at[1])][k] = squeeze(value[rows - RAD:])
    all_greeted(found)
    copies = transfers(found, pieces, halos, send_sems, recv_sems)
    start_all(copies)

    def solve_group(group, _):
        def load(b, cut):
            return windows[0, group * GROUP + b, cut, :], windows[1, group * GROUP + b, cut, :]

        def store(b, cut, current):
            cur[group * GROUP + b, cut, :] = current

        solve(load, store)
        return 0

    lax.fori_loop(0, slots // GROUP, solve_group, 0)
    finish_all(copies, landings(found, pieces, halos, send_sems, recv_sems))
    for at in SHIFTS:
        outs[at][...] = halos[at][...]


def return_kernel(*refs):
    pieces, outs, halos = (dict(zip(SHIFTS, refs[8 * k:8 * k + 8])) for k in range(3))
    send_sems, recv_sems = refs[24:]
    found = neighbours()
    for at in SHIFTS:
        halos[at][...] = jnp.zeros_like(halos[at])
    greet(found)
    all_greeted(found)
    copies = transfers(found, pieces, halos, send_sems, recv_sems)
    start_all(copies)
    finish_all(copies, landings(found, pieces, halos, send_sems, recv_sems))
    for at in SHIFTS:
        outs[at][...] = halos[at][...]


def border_kernel(rows, cols, centers, live, inner_cur, *refs):
    raw, halos = refs[:3], dict(zip(SHIFTS, refs[3:11]))
    out, outs = refs[11], dict(zip(SHIFTS, refs[12:20]))
    bufs, sems, order, ext, acc, out_sem, staged, solved = refs[20:23], *refs[23:30]
    clear, solve = solver_parts(refs[30:])

    def copies(slot):
        top, left = corner_of(centers, slot, rows, cols)
        row, col = clamped(top, left, rows, cols)
        return [
            pltpu.make_async_copy(
                src.at[pl.ds(row, TALL), pl.ds(col, WIDE)],
                dst.at[slot, pl.ds(RAD, TALL), :],
                sems.at[k, slot],
            )
            for k, (src, dst) in enumerate(zip(raw, bufs))
        ]

    def classify(slot, count):
        top, left = corner_of(centers, slot, rows, cols)
        outer = jnp.logical_not(is_inner(top, left, rows, cols))

        @pl.when(outer)
        def _():
            order[count] = slot
            for copy in copies(slot):
                copy.start()

        return count + outer.astype(jnp.int32)

    count = lax.fori_loop(0, live[0], classify, jnp.int32(0))
    acc[...] = jnp.zeros_like(acc)
    clear()
    spans = spans_of(rows, cols)
    for which in range(2):
        for dr in (-1, 1):
            ext[which, spans[dr][0], spans[0][1]] = halos[(dr, 0)][which]
        for dr in (-1, 0, 1):
            start, stop = spans[dr][0].start, spans[dr][0].stop
            middle = (start + stop) // 2
            for dc in (-1, 1):
                split = to_high if dc < 0 else to_low
                first, second = split(halos[(dr, dc)][which])
                ext[which, start:middle, spans[dc][1]] = first
                ext[which, middle:stop, spans[dc][1]] = second

    row_id = lax.broadcasted_iota(jnp.int32, (SIDE, SIDE), 0)
    col_id = lax.broadcasted_iota(jnp.int32, (SIDE, SIDE), 1)

    def fetch(slot):
        top, left = corner_of(centers, slot, rows, cols)
        row, col = clamped(top, left, rows, cols)
        take = pl.ds(pl.multiple_of((RAD + top - row) // 8 * 8, 8), TALL)
        res, source, target = (buf[slot, take, :] for buf in bufs)
        res, mark = turn_own(res, source, target, lax.rem(RAD + top - row, 8), col - left)
        at_row, at_col = row_id + top, col_id + left
        own = (at_row >= 0) & (at_row < rows) & (at_col >= 0) & (at_col < cols)
        base = pl.multiple_of((left + LANES) // LANES * LANES, LANES)
        back = lax.rem(WIDE + base - left - LANES, WIDE)
        span = pl.ds(pl.multiple_of((top + RAD) // 8 * 8, 8), TALL)
        outer = [
            cut_rows(pltpu.roll(ext[k, span, pl.ds(base, WIDE)], back, 1)[:, :SIDE], lax.rem(top + RAD, 8))
            for k in range(2)
        ]
        res = jnp.where(own, res, outer[0])
        return jnp.where(res > 0.0, res, FAR), jnp.where(own, mark, outer[1])

    def solve_group(group, _):
        def ready(b, _):
            at = group * GROUP + b
            slot = order[jnp.minimum(at, count - 1)]

            @pl.when(at < count)
            def _():
                for copy in copies(slot):
                    copy.wait()

            staged[0, b], staged[1, b] = fetch(slot)
            return 0

        def store(b, cut, current):
            solved[b, cut, :] = current

        def done(b, _):
            top, left = corner_of(centers, order[group * GROUP + b], rows, cols)
            add_window(acc, solved[b], top, left)
            return 0

        lax.fori_loop(0, GROUP, ready, 0)
        solve(lambda b, cut: (staged[0, b, cut, :], staged[1, b, cut, :]), store)
        lax.fori_loop(0, jnp.minimum(count - group * GROUP, GROUP), done, 0)
        return 0

    lax.fori_loop(0, (count + GROUP - 1) // GROUP, solve_group, 0)

    def place(slot, _):
        top, left = corner_of(centers, slot, rows, cols)

        @pl.when(is_inner(top, left, rows, cols))
        def _():
            add_window(acc, inner_cur[slot], top, left)

        return 0

    lax.fori_loop(0, live[0], place, 0)
    copy = pltpu.make_async_copy(acc.at[pl.ds(RAD, rows), pl.ds(LANES, cols)], out, out_sem)
    copy.start()
    for dr in (-1, 1):
        outs[(dr, 0)][...] = acc[spans[dr][0], spans[0][1]]
    for dr in (-1, 0, 1):
        for dc in (-1, 1):
            tile = acc[spans[dr][0], spans[dc][1]]
            outs[(dr, dc)][...] = pack_high(tile) if dc < 0 else pack_low(tile)
    copy.wait()


def fold_kernel(rows, cols, *refs):
    halos = dict(zip(SHIFTS, refs[1:9]))
    out, upper, lower, left, right, sems = refs[9:]
    last = cols - LANES
    inner_rows = rows - SIDE
    places = (
        (upper, pl.ds(0, RAD), pl.ds(0, cols)),
        (lower, pl.ds(rows - RAD, RAD), pl.ds(0, cols)),
        (left, pl.ds(RAD, inner_rows), pl.ds(0, LANES)),
        (right, pl.ds(RAD, inner_rows), pl.ds(last, LANES)),
    )
    fetch = [pltpu.make_async_copy(out.at[r, c], buf, sems.at[0, k]) for k, (buf, r, c) in enumerate(places)]
    store = [pltpu.make_async_copy(buf, out.at[r, c], sems.at[1, k]) for k, (buf, r, c) in enumerate(places)]
    for copy in fetch:
        copy.start()

    def spread(dr, dc):
        first, second = (to_low if dc < 0 else to_high)(halos[(dr, dc)][...])
        low = lane_ids(first.shape) < RAD
        keep = low if dc < 0 else jnp.logical_not(low)
        return jnp.where(keep, first, 0.0), jnp.where(keep, second, 0.0)

    for copy in fetch:
        copy.wait()
    half = rows // 2
    for dc, buf, at in ((-1, left, 0), (1, right, last)):
        first, second = spread(0, dc)
        buf[0:half - RAD] = buf[0:half - RAD] + first[RAD:]
        buf[half - RAD:inner_rows] = buf[half - RAD:inner_rows] + second[:half - RAD]
        upper[:, at:at + LANES] = upper[:, at:at + LANES] + first[:RAD]
        lower[:, at:at + LANES] = lower[:, at:at + LANES] + second[half - RAD:]
        for dr, strip in ((-1, upper), (1, lower)):
            one, two = spread(dr, dc)
            strip[:RAD // 2, at:at + LANES] = strip[:RAD // 2, at:at + LANES] + one
            strip[RAD // 2:, at:at + LANES] = strip[RAD // 2:, at:at + LANES] + two
    upper[...] = upper[...] + halos[(-1, 0)][...]
    lower[...] = lower[...] + halos[(1, 0)][...]
    for copy in store:
        copy.start()
    for copy in store:
        copy.wait()


def local(resistance, source_mask, target_mask, centers, live_counts):
    rows, cols = resistance.shape
    slots = centers.shape[0]
    f32, i32 = jnp.float32, jnp.int32
    smem = pl.BlockSpec(memory_space=pltpu.SMEM)
    vmem = pl.BlockSpec(memory_space=pltpu.VMEM)
    hbm = pl.BlockSpec(memory_space=pltpu.HBM)

    shapes = {
        at: (RAD if at[0] else rows, cols) if at[1] == 0 else ((RAD if at[0] else rows) // 2, LANES) for at in SHIFTS
    }
    pairs = [pltpu.VMEM((2, *shapes[at]), f32) for at in SHIFTS]
    strips = [pltpu.VMEM(shapes[at], f32) for at in SHIFTS]
    state = solver_state()
    stage = [pltpu.VMEM((2, GROUP, SIDE, SIDE), f32), pltpu.VMEM((GROUP, SIDE, SIDE), f32)]
    kinds = (f32, i32, i32)
    frame_shapes = ((rows, LANES), (rows, LANES), (RAD, cols), (RAD, cols))

    windows = pl.pallas_call(
        functools.partial(cut_kernel, rows, cols),
        out_shape=jax.ShapeDtypeStruct((2, slots, SIDE, SIDE), f32),
        in_specs=[smem, smem, hbm, hbm, hbm],
        out_specs=vmem,
        scratch_shapes=[pltpu.VMEM((slots, TALL, WIDE), kind) for kind in kinds]
        + [pltpu.SemaphoreType.DMA((3, slots))],
        compiler_params=pltpu.CompilerParams(vmem_limit_bytes=57 << 20),
        name="cut",
    )(centers, live_counts, resistance, source_mask, target_mask)

    inner_cur, *halos = pl.pallas_call(
        functools.partial(inner_kernel, rows, cols),
        out_shape=[jax.ShapeDtypeStruct((slots, SIDE, SIDE), f32)]
        + [jax.ShapeDtypeStruct((2, *shapes[at]), f32) for at in SHIFTS],
        in_specs=[vmem, hbm, hbm, hbm],
        out_specs=[vmem] * 9,
        scratch_shapes=pairs
        + pairs
        + [pltpu.VMEM(shape, kind) for shape in frame_shapes for kind in kinds]
        + [pltpu.SemaphoreType.DMA((4, 3)), pltpu.SemaphoreType.DMA((8,)), pltpu.SemaphoreType.DMA((8,))]
        + state,
        compiler_params=pltpu.CompilerParams(vmem_limit_bytes=51 << 20, collective_id=0, has_side_effects=True),
        name="inner",
    )(windows, resistance, source_mask, target_mask)

    merged, *currents = pl.pallas_call(
        functools.partial(border_kernel, rows, cols),
        out_shape=[jax.ShapeDtypeStruct((rows, cols), f32)]
        + [jax.ShapeDtypeStruct(shapes[at], f32) for at in SHIFTS],
        in_specs=[smem, smem, vmem, hbm, hbm, hbm] + [vmem] * 8,
        out_specs=[hbm] + [vmem] * 8,
        scratch_shapes=[pltpu.VMEM((slots, TALL + SIDE, WIDE), kind) for kind in kinds]
        + [
            pltpu.SemaphoreType.DMA((3, slots)),
            pltpu.SMEM((slots,), i32),
            pltpu.VMEM((2, rows + SIDE, cols + WIDE), f32),
            pltpu.VMEM((rows + SIDE, cols + WIDE), f32),
            pltpu.SemaphoreType.DMA,
        ]
        + stage
        + state,
        compiler_params=pltpu.CompilerParams(vmem_limit_bytes=58 << 20),
        name="border",
    )(centers, live_counts, inner_cur, resistance, source_mask, target_mask, *halos)

    back = pl.pallas_call(
        return_kernel,
        out_shape=[jax.ShapeDtypeStruct(shapes[at], f32) for at in SHIFTS],
        in_specs=[vmem] * 8,
        out_specs=[vmem] * 8,
        scratch_shapes=strips + [pltpu.SemaphoreType.DMA((8,)), pltpu.SemaphoreType.DMA((8,))],
        compiler_params=pltpu.CompilerParams(vmem_limit_bytes=8 << 20, collective_id=1, has_side_effects=True),
        name="give_back",
    )(*currents)
    out_shape = jax.ShapeDtypeStruct((rows, cols), f32)

    return pl.pallas_call(
        functools.partial(fold_kernel, rows, cols),
        out_shape=out_shape,
        in_specs=[hbm] + [vmem] * 8,
        out_specs=hbm,
        scratch_shapes=[
            pltpu.VMEM((RAD, cols), f32),
            pltpu.VMEM((RAD, cols), f32),
            pltpu.VMEM((rows - SIDE, LANES), f32),
            pltpu.VMEM((rows - SIDE, LANES), f32),
            pltpu.SemaphoreType.DMA((2, 4)),
        ],
        input_output_aliases={0: 0},
        compiler_params=pltpu.CompilerParams(vmem_limit_bytes=16 << 20),
        name="fold",
    )(merged, *back)


def solution(mesh):
    return jax.shard_map(
        local,
        mesh=mesh,
        in_specs=(
            P("row", "col"),
            P("row", "col"),
            P("row", "col"),
            P(("row", "col"), None),
            P(("row", "col")),
        ),
        out_specs=P("row", "col"),
        check_vma=False,
    )
```

```python
import functools

import jax
import jax.numpy as jnp
from jax import lax
from jax.experimental import pallas as pl
from jax.experimental.pallas import tpu as pltpu
from jax.sharding import PartitionSpec as P

RAD = 64
SIDE = 2 * RAD
ITERS = 24
LEAKAGE = 0.02
FAR = 1e37
GROUP = 8
LANES = 128
TALL = SIDE + 8
WIDE = 2 * LANES
SHIFTS = ((0, -1), (0, 1), (-1, 0), (1, 0), (-1, -1), (-1, 1), (1, -1), (1, 1))


def roll(value, shift, axis):
    return pltpu.roll(value, shift % value.shape[axis], axis)


def lane_ids(shape):
    return lax.broadcasted_iota(jnp.int32, shape, 1)


def to_low(packed):
    return packed, roll(packed, RAD, 1)


def to_high(packed):
    return roll(packed, RAD, 1), packed


def pack_low(tile):
    half = tile.shape[0] // 2
    first, second = tile[:half], tile[half:]
    return jnp.where(lane_ids(first.shape) < RAD, first, roll(second, RAD, 1))


def pack_high(tile):
    half = tile.shape[0] // 2
    first, second = tile[:half], tile[half:]
    return jnp.where(lane_ids(first.shape) < RAD, roll(first, RAD, 1), second)


def neighbours():
    row, col = lax.axis_index("row"), lax.axis_index("col")
    rows, cols = lax.axis_size("row"), lax.axis_size("col")
    found = {}
    for (dr, dc) in SHIFTS:
        r, c = row + dr, col + dc
        found[(dr, dc)] = ((r >= 0) & (r < rows) & (c >= 0) & (c < cols), (r, c))
    return found


def greet(found):
    barrier = pltpu.get_barrier_semaphore()
    for at in SHIFTS:
        exists, device = found[at]

        @pl.when(exists)
        def _():
            pl.semaphore_signal(barrier, inc=1, device_id=device, device_id_type=pl.DeviceIdType.MESH)


def all_greeted(found):
    count = sum(found[at][0].astype(jnp.int32) for at in SHIFTS)
    pl.semaphore_wait(pltpu.get_barrier_semaphore(), count)


def transfers(found, pieces, halos, send_sems, recv_sems):
    made = []
    for k, at in enumerate(SHIFTS):
        exists, device = found[at]
        back = (-at[0], -at[1])
        made.append((exists, pltpu.make_async_remote_copy(
            src_ref=pieces[at],
            dst_ref=halos[back],
            send_sem=send_sems.at[k],
            recv_sem=recv_sems.at[SHIFTS.index(back)],
            device_id=device,
            device_id_type=pl.DeviceIdType.MESH,
        )))
    return made


def landings(found, pieces, halos, send_sems, recv_sems):
    made = []
    for k, at in enumerate(SHIFTS):
        exists, device = found[at]
        made.append((exists, pltpu.make_async_remote_copy(
            src_ref=pieces[at],
            dst_ref=halos[at],
            send_sem=send_sems.at[k],
            recv_sem=recv_sems.at[k],
            device_id=device,
            device_id_type=pl.DeviceIdType.MESH,
        )))
    return made


def start_all(copies):
    for exists, copy in copies:
        pl.when(exists)(copy.start)


def finish_all(copies, arrivals):
    for exists, copy in copies:
        pl.when(exists)(copy.wait_send)
    for exists, copy in arrivals:
        pl.when(exists)(copy.wait_recv)


def corner_of(centers, slot, rows, cols):
    return lax.rem(centers[slot, 0], rows) - RAD, lax.rem(centers[slot, 1], cols) - RAD


def is_inner(top, left, rows, cols):
    return (top >= 0) & (top <= rows - SIDE) & (left >= 0) & (left <= cols - SIDE)


def clamped(top, left, rows, cols):
    row = jnp.clip((top + RAD) // 8 * 8 - RAD, 0, rows - TALL)
    col = jnp.clip((left + LANES) // LANES * LANES - LANES, 0, cols - WIDE)
    return pl.multiple_of(row, 8), pl.multiple_of(col, LANES)


def total(values):
    return jnp.sum(jnp.sum(values, axis=0, keepdims=True), axis=1, keepdims=True)


def cut_rows(value, skip):
    return pltpu.roll(value, lax.rem(TALL - skip, TALL), 0)[:SIDE]


def add_window(acc, current, top, left):
    col = pl.multiple_of((left + LANES) // LANES * LANES, LANES)
    shift = left + LANES - col
    wide = jnp.concatenate([current, jnp.zeros_like(current)], axis=1)
    wide = pltpu.roll(wide, shift, 1)
    wide = jnp.concatenate([wide, jnp.zeros((8, WIDE), jnp.float32)], axis=0)
    wide = pltpu.roll(wide, lax.rem(top + RAD, 8), 0)
    rows = pl.ds(pl.multiple_of((top + RAD) // 8 * 8, 8), TALL)
    acc[rows, pl.ds(col, WIDE)] = acc[rows, pl.ds(col, WIDE)] + wide


PLANES = 4
CHUNK = 64
SEGMENTS = SIDE // PLANES
EIGHTS = tuple(slice(8 * k, 8 * k + 8) for k in range(SIDE // 8))


def lanes_of(shape):
    return lax.broadcasted_iota(jnp.int32, shape, 1)


def interleave(shape, transposed):
    row, col = (lax.broadcasted_iota(jnp.int32, shape, axis) for axis in (0, 1))
    if transposed:
        row, col = col, row
    window, place = row // SIDE, row % SIDE
    return (col == (place % PLANES) * SIDE + window * SEGMENTS + place // PLANES).astype(jnp.bfloat16)


def halves(value):
    high = value.astype(jnp.bfloat16)
    return high, (value - high.astype(jnp.float32)).astype(jnp.bfloat16)


def mixed(parts, table):
    found = jnp.dot(jnp.concatenate(parts, axis=0), table[...], preferred_element_type=jnp.float32)
    size = parts[0].shape[0]
    return [found[size * n:size * n + size] for n in range(len(parts))]


def quad_state():
    f32 = jnp.float32
    planes = pltpu.VMEM((PLANES, SIDE, SIDE), f32)
    padded = pltpu.VMEM((PLANES, SIDE + 16, SIDE), f32)
    tile = pltpu.VMEM((SIDE, SIDE), f32)
    table = pltpu.VMEM((ITERS, 8, SIDE), f32)
    return (
        [padded, padded, pltpu.VMEM((ITERS, PLANES, SIDE, SIDE), f32), planes]
        + [padded, planes, tile]
        + [tile, tile]
        + [padded, planes, planes, padded, padded, planes]
        + [table, table]
    )


def solver_state(group):
    wide = PLANES * SIDE
    return quad_state() * (group // PLANES) + [pltpu.VMEM((2, wide, wide), jnp.bfloat16)]


def quad_parts(state):
    even, odd, hist, t_s, vert, hori, hori_in, edge_r, edge_l, isd_s, inj_s, gnd_s, v_s, res_s, h_s, tail_s, link_s = state
    f32 = jnp.float32
    mid = tuple(slice(8 + 8 * k, 16 + 8 * k) for k in range(SIDE // 8))
    low = tuple(slice(9 + 8 * k, 17 + 8 * k) for k in range(SIDE // 8))
    upp = tuple(slice(7 + 8 * k, 15 + 8 * k) for k in range(SIDE // 8))
    blocks = range(SIDE // 8)
    lane = lanes_of((8, SIDE))
    row8 = lax.broadcasted_iota(jnp.int32, (8, SIDE), 0)

    def clear():
        zero = jnp.zeros((8, SIDE), f32)
        for pad in (even, odd, vert, isd_s, v_s, res_s):
            for p in range(PLANES):
                pad[p, 0:8, :] = zero
                pad[p, 8 + SIDE:16 + SIDE, :] = zero

    def refresh_edges(cur):
        for k in blocks:
            edge_r[EIGHTS[k], :] = roll(cur[0, mid[k], :], -1, 1)
            edge_l[EIGHTS[k], :] = roll(cur[PLANES - 1, mid[k], :], 1, 1)

    def operate(cur):
        gammas, deltas = [None] * PLANES, [None] * PLANES
        for k in blocks:
            here = [cur[p, mid[k], :] for p in range(PLANES)]
            out = [hori[p, EIGHTS[k], :] for p in range(PLANES)]
            for p in (1, 2, 0, 3):
                right = here[p + 1] if p < PLANES - 1 else edge_r[EIGHTS[k], :]
                left = here[p - 1] if p else edge_l[EIGHTS[k], :]
                back = out[p - 1] if p else hori_in[EIGHTS[k], :]
                beside = vert[p, mid[k], :] * cur[p, low[k], :] + vert[p, upp[k], :] * cur[p, upp[k], :]
                beside = beside + (out[p] * right + back * left)
                t_s[p, EIGHTS[k], :] = beside
                one, two = here[p] * here[p], here[p] * beside
                gammas[p] = one if k == 0 else gammas[p] + one
                deltas[p] = two if k == 0 else deltas[p] + two
        return (gammas[0] + gammas[1]) + (gammas[2] + gammas[3]), (deltas[0] + deltas[1]) + (deltas[2] + deltas[3])

    def down_sum(part):
        for shift in (4, 2, 1):
            part = part + roll(part, shift, 0)
        return part

    def total_of(sums):
        mine = lane // SEGMENTS == row8 % PLANES
        first = row8 < PLANES
        both = jnp.where(first, down_sum(sums[0]), down_sum(sums[1]))
        both = jnp.where(mine, jnp.sum(jnp.where(mine, both, 0.0), axis=1, keepdims=True), 0.0)
        return down_sum(jnp.where(first, both, 0.0)), down_sum(jnp.where(first, 0.0, both))

    def prepare(load, table):
        for r in range(0, SIDE, CHUNK):
            cut = slice(r, r + CHUNK)
            loaded = [load(w, cut) for w in range(PLANES)]
            res = jnp.concatenate([pair[0] for pair in loaded], axis=1)
            mark = jnp.concatenate([pair[1] for pair in loaded], axis=1)
            high, low_part, mark = mixed([*halves(res), mark.astype(jnp.bfloat16)], table)
            res = high + low_part
            signed = mark / res
            for p in range(PLANES):
                span = slice(SIDE * p, SIDE * p + SIDE)
                res_s[p, 8 + r:8 + r + CHUNK, :] = res[:, span]
                inject = jnp.maximum(signed[:, span], 0.0)
                if p == 0 and r <= RAD < r + CHUNK:
                    at = lax.broadcasted_iota(jnp.int32, (CHUNK, SIDE), 0) == RAD - r
                    spot = lanes_of((CHUNK, SIDE)) % SEGMENTS == RAD // PLANES
                    inject = inject + (at & spot).astype(f32)
                inj_s[p, cut, :] = inject
                gnd_s[p, cut, :] = jnp.maximum(-signed[:, span], 0.0)
        ends = lane % SEGMENTS == SEGMENTS - 1
        bottom = row8 == 7
        for k in blocks:
            for p in range(PLANES):
                here = res_s[p, mid[k], :]
                under = res_s[p, low[k], :]
                if k == len(EIGHTS) - 1:
                    vertical = jnp.where(bottom, 0.0, 2.0 / (here + jnp.where(bottom, FAR, under)))
                else:
                    vertical = 2.0 / (here + under)
                v_s[p, mid[k], :] = vertical
                if p < PLANES - 1:
                    h_s[p, EIGHTS[k], :] = 2.0 / (here + res_s[p + 1, mid[k], :])
                else:
                    horizontal = jnp.where(ends, 0.0, 2.0 / (here + roll(res_s[0, mid[k], :], -1, 1)))
                    h_s[p, EIGHTS[k], :] = horizontal
                    edge_l[EIGHTS[k], :] = roll(horizontal, 1, 1)
        for k in blocks:
            for p in range(PLANES):
                before = h_s[p - 1, EIGHTS[k], :] if p else edge_l[EIGHTS[k], :]
                diagonal = v_s[p, mid[k], :] + v_s[p, upp[k], :] + (h_s[p, EIGHTS[k], :] + before)
                isd_s[p, mid[k], :] = 1.0 / jnp.sqrt(diagonal + gnd_s[p, EIGHTS[k], :] + LEAKAGE)
        for k in blocks:
            for p in range(PLANES):
                isd = isd_s[p, mid[k], :]
                vert[p, mid[k], :] = v_s[p, mid[k], :] * isd * isd_s[p, low[k], :]
                if p < PLANES - 1:
                    hori[p, EIGHTS[k], :] = h_s[p, EIGHTS[k], :] * isd * isd_s[p + 1, mid[k], :]
                else:
                    scaled = h_s[p, EIGHTS[k], :] * isd * roll(isd_s[0, mid[k], :], -1, 1)
                    hori[p, EIGHTS[k], :] = scaled
                    hori_in[EIGHTS[k], :] = roll(scaled, 1, 1)
                first = inj_s[p, EIGHTS[k], :] * isd
                even[p, mid[k], :] = first
                hist[0, p, EIGHTS[k], :] = first
        refresh_edges(even)
        return operate(even)

    def settle(j, sums, gamma_inv_before, pivot_inv, weight):
        gamma, delta = sums
        gamma_inv = 1.0 / gamma
        mean = delta * gamma_inv
        ratio = gamma * gamma_inv_before
        link = ratio * pivot_inv
        pivot_inv = 1.0 / (1.0 - mean - link)
        weight = weight * pivot_inv
        tail_s[j] = weight
        link_s[j] = link
        return mean, ratio, gamma_inv, pivot_inv, weight

    def update(j, way, mean, ratio):
        cur, new = (odd, even) if way else (even, odd)
        for p in (0, 3, 1, 2):
            for k in blocks:
                fresh = t_s[p, EIGHTS[k], :] - mean * cur[p, mid[k], :]
                if ratio is not None:
                    fresh = fresh - ratio * new[p, mid[k], :]
                new[p, mid[k], :] = fresh
                hist[j + 1, p, EIGHTS[k], :] = fresh
                if p == 0:
                    edge_r[EIGHTS[k], :] = roll(fresh, -1, 1)
                if p == PLANES - 1:
                    edge_l[EIGHTS[k], :] = roll(fresh, 1, 1)
        return operate(new)

    def coefficients():
        factor = tail_s[ITERS - 1]
        for j in reversed(range(1, ITERS)):
            ahead = tail_s[j - 1] + link_s[j] * factor
            tail_s[j] = factor
            factor = ahead
        tail_s[0] = factor

    def voltages():
        def one(p, _):
            for half in range(2):
                found = [None] * 8
                for j in range(ITERS):
                    factor = tail_s[j]
                    for i in range(8):
                        term = factor * hist[j, p, EIGHTS[8 * half + i], :]
                        found[i] = term if found[i] is None else found[i] + term
                for i in range(8):
                    even[p, mid[8 * half + i], :] = found[i] * isd_s[p, mid[8 * half + i], :]
            return 0

        lax.fori_loop(0, PLANES, one, 0)

    def finish(put, table):
        cur = even
        for k in blocks:
            edge_r[EIGHTS[k], :] = roll(cur[0, mid[k], :], -1, 1)
        for k in blocks:
            for p in range(PLANES):
                volts = cur[p, mid[k], :]
                res_s[p, mid[k], :] = v_s[p, mid[k], :] * jnp.abs(volts - cur[p, low[k], :])
                right = cur[p + 1, mid[k], :] if p < PLANES - 1 else edge_r[EIGHTS[k], :]
                flow = h_s[p, EIGHTS[k], :] * jnp.abs(volts - right)
                t_s[p, EIGHTS[k], :] = flow
                if p == PLANES - 1:
                    edge_l[EIGHTS[k], :] = roll(flow, 1, 1)

        for r in range(0, SIDE, CHUNK):
            cut = slice(r, r + CHUNK)
            pieces = []
            for p in range(PLANES):
                flow = res_s[p, 8 + r:8 + r + CHUNK, :] + res_s[p, 7 + r:7 + r + CHUNK, :] + t_s[p, cut, :]
                flow = flow + (t_s[p - 1, cut, :] if p else edge_l[cut, :])
                pieces.append(0.5 * (flow + inj_s[p, cut, :] + gnd_s[p, cut, :] * jnp.abs(cur[p, 8 + r:8 + r + CHUNK, :])))
            high, low_part = mixed(halves(jnp.concatenate(pieces, axis=1)), table)
            for w in range(PLANES):
                span = slice(SIDE * w, SIDE * w + SIDE)
                put(w, cut, high[:, span] + low_part[:, span])

    return clear, prepare, total_of, operate, settle, update, coefficients, voltages, finish


def solver_parts(state, group):
    table = state[-1]
    count = group // PLANES
    size = (len(state) - 1) // count
    quads = [quad_parts(state[size * q:size * q + size]) for q in range(count)]

    def clear():
        for quad in quads:
            quad[0]()
        for way in range(2):
            table[way] = interleave(table.shape[1:], way == 1)

    def solve(load, store):
        one = jnp.ones((8, SIDE), jnp.float32)
        carry = []
        for q, (_, prepare, total_of, *_) in enumerate(quads):
            sums = prepare(lambda w, cut, q=q: load(PLANES * q + w, cut), table.at[0])
            carry.append((sums if q else total_of(sums), 0.0 * one, 0.0 * one, one))

        def step(j, way, carry, first=False):
            after = []
            for q, (_, _, total_of, operate, settle, update, *_) in enumerate(quads):
                sums, *rest = carry[q]
                if q:
                    sums = total_of(sums)
                mean, ratio, *rest = settle(j, sums, *rest)
                sums = update(j, way, mean, None if first else ratio)
                after.append((sums if q else total_of(sums), *rest))
            return after

        def steps(i, carry):
            return tuple(step(2 * i + 2, 0, step(2 * i + 1, 1, carry)))

        carry = tuple(step(0, 0, carry, True))
        carry = lax.fori_loop(0, (ITERS - 2) // 2, steps, carry)
        for q, (_, _, total_of, _, settle, _, coefficients, *_) in enumerate(quads):
            settle(ITERS - 1, total_of(carry[q][0]) if q else carry[q][0], *carry[q][1:])
            coefficients()
        for q, (*_, voltages, finish) in enumerate(quads):
            voltages()
            finish(lambda w, cut, tile, q=q: store(PLANES * q + w, cut, tile), table.at[1])

    return clear, solve


def spans_of(rows, cols):
    return {
        -1: (slice(0, RAD), slice(0, LANES)),
        0: (slice(RAD, RAD + rows), slice(LANES, LANES + cols)),
        1: (slice(RAD + rows, SIDE + rows), slice(LANES + cols, WIDE + cols)),
    }


def turn_own(res, source, target, skip, turn):
    source, target = source.astype(jnp.float32), target.astype(jnp.float32)
    mark = source - target * (1.0 - source)
    turn = lax.rem(WIDE + turn, WIDE)
    res = cut_rows(pltpu.roll(res, turn, 1)[:, :SIDE], skip)
    mark = cut_rows(pltpu.roll(mark, turn, 1)[:, :SIDE], skip)
    return res, mark


def cut_kernel(rows, cols, centers, live, *refs):
    raw, out, bufs, sems = refs[:3], refs[3], refs[4:7], refs[7]

    def place(slot):
        top, left = corner_of(centers, slot, rows, cols)
        return top, left, *clamped(top, left, rows, cols)

    def copies(slot):
        _, _, row, col = place(slot)
        return [
            pltpu.make_async_copy(src.at[pl.ds(row, TALL), pl.ds(col, WIDE)], dst.at[slot], sems.at[k, slot])
            for k, (src, dst) in enumerate(zip(raw, bufs))
        ]

    def begin(slot, _):
        for copy in copies(slot):
            copy.start()
        return 0

    def cut(slot, _):
        for copy in copies(slot):
            copy.wait()
        top, left, row, col = place(slot)
        res, mark = turn_own(*(buf[slot] for buf in bufs), top - row, col - left)
        out[0, slot] = res
        out[1, slot] = mark
        return 0

    def blank(slot, _):
        out[0, slot] = jnp.ones((SIDE, SIDE), jnp.float32)
        out[1, slot] = jnp.zeros((SIDE, SIDE), jnp.float32)
        return 0

    lax.fori_loop(0, live[0], begin, 0)
    lax.fori_loop(live[0], out.shape[1], blank, 0)
    lax.fori_loop(0, live[0], cut, 0)


def inner_kernel(rows, cols, windows, *refs):
    raw = refs[:3]
    cur, outs = refs[3], dict(zip(SHIFTS, refs[4:12]))
    pieces, halos = dict(zip(SHIFTS, refs[12:20])), dict(zip(SHIFTS, refs[20:28]))
    frames = [refs[28 + 3 * k:31 + 3 * k] for k in range(4)]
    sems, send_sems, recv_sems = refs[40:43]
    clear, solve = solver_parts(refs[43:], GROUP)
    slots = windows.shape[1]
    found = neighbours()
    clear()

    everything = pl.ds(0, rows)
    places = (
        (everything, pl.ds(0, LANES)),
        (everything, pl.ds(cols - LANES, LANES)),
        (pl.ds(0, RAD), pl.ds(0, cols)),
        (pl.ds(rows - RAD, RAD), pl.ds(0, cols)),
    )
    frame_copies = [
        [pltpu.make_async_copy(raw[k].at[places[f]], frames[f][k], sems.at[f, k]) for k in range(3)]
        for f in range(4)
    ]
    for copy in sum(frame_copies, []):
        copy.start()
    for at in SHIFTS:
        halos[at][...] = jnp.zeros_like(halos[at])
    greet(found)

    def strengths(frame, cut=slice(None)):
        res, source, target = (ref[cut] for ref in frame)
        source, target = source.astype(jnp.float32), target.astype(jnp.float32)
        return res, source - target * (1.0 - source)

    for f, at in enumerate(((0, -1), (0, 1), (-1, 0), (1, 0))):
        for copy in frame_copies[f]:
            copy.wait()
        for k, value in enumerate(strengths(frames[f])):
            if at[1] == 0:
                pieces[at][k] = value
            else:
                squeeze = pack_low if at[1] < 0 else pack_high
                pieces[at][k] = squeeze(value)
                pieces[(-1, at[1])][k] = squeeze(value[:RAD])
                pieces[(1, at[1])][k] = squeeze(value[rows - RAD:])
    all_greeted(found)
    copies = transfers(found, pieces, halos, send_sems, recv_sems)
    start_all(copies)

    def solve_group(group, _):
        def load(b, cut):
            return windows[0, group * GROUP + b, cut, :], windows[1, group * GROUP + b, cut, :]

        def store(b, cut, current):
            cur[group * GROUP + b, cut, :] = current

        solve(load, store)
        return 0

    lax.fori_loop(0, slots // GROUP, solve_group, 0)
    finish_all(copies, landings(found, pieces, halos, send_sems, recv_sems))
    for at in SHIFTS:
        outs[at][...] = halos[at][...]


def return_kernel(*refs):
    pieces, outs, halos = (dict(zip(SHIFTS, refs[8 * k:8 * k + 8])) for k in range(3))
    send_sems, recv_sems = refs[24:]
    found = neighbours()
    for at in SHIFTS:
        halos[at][...] = jnp.zeros_like(halos[at])
    greet(found)
    all_greeted(found)
    copies = transfers(found, pieces, halos, send_sems, recv_sems)
    start_all(copies)
    finish_all(copies, landings(found, pieces, halos, send_sems, recv_sems))
    for at in SHIFTS:
        outs[at][...] = halos[at][...]


def border_kernel(rows, cols, centers, live, inner_cur, *refs):
    raw, halos = refs[:3], dict(zip(SHIFTS, refs[3:11]))
    out, outs = refs[11], dict(zip(SHIFTS, refs[12:20]))
    bufs, sems, order, ext, acc, out_sem, staged, solved = refs[20:23], *refs[23:30]
    clear, solve = solver_parts(refs[30:], PLANES)

    def copies(slot, at):
        top, left = corner_of(centers, slot, rows, cols)
        row, col = clamped(top, left, rows, cols)
        return [
            pltpu.make_async_copy(
                src.at[pl.ds(row, TALL), pl.ds(col, WIDE)],
                dst.at[at, pl.ds(RAD, TALL), :],
                sems.at[k, at],
            )
            for k, (src, dst) in enumerate(zip(raw, bufs))
        ]

    def classify(slot, count):
        top, left = corner_of(centers, slot, rows, cols)
        outer = jnp.logical_not(is_inner(top, left, rows, cols))

        @pl.when(outer)
        def _():
            order[count] = slot

        return count + outer.astype(jnp.int32)

    count = lax.fori_loop(0, live[0], classify, jnp.int32(0))
    acc[...] = jnp.zeros_like(acc)
    clear()
    spans = spans_of(rows, cols)
    for which in range(2):
        for dr in (-1, 1):
            ext[which, spans[dr][0], spans[0][1]] = halos[(dr, 0)][which]
        for dr in (-1, 0, 1):
            start, stop = spans[dr][0].start, spans[dr][0].stop
            middle = (start + stop) // 2
            for dc in (-1, 1):
                split = to_high if dc < 0 else to_low
                first, second = split(halos[(dr, dc)][which])
                ext[which, start:middle, spans[dc][1]] = first
                ext[which, middle:stop, spans[dc][1]] = second

    row_id = lax.broadcasted_iota(jnp.int32, (SIDE, SIDE), 0)
    col_id = lax.broadcasted_iota(jnp.int32, (SIDE, SIDE), 1)

    def fetch(slot, b):
        top, left = corner_of(centers, slot, rows, cols)
        row, col = clamped(top, left, rows, cols)
        take = pl.ds(pl.multiple_of((RAD + top - row) // 8 * 8, 8), TALL)
        res, source, target = (buf[b, take, :] for buf in bufs)
        res, mark = turn_own(res, source, target, lax.rem(RAD + top - row, 8), col - left)
        at_row, at_col = row_id + top, col_id + left
        own = (at_row >= 0) & (at_row < rows) & (at_col >= 0) & (at_col < cols)
        base = pl.multiple_of((left + LANES) // LANES * LANES, LANES)
        back = lax.rem(WIDE + base - left - LANES, WIDE)
        span = pl.ds(pl.multiple_of((top + RAD) // 8 * 8, 8), TALL)
        outer = [
            cut_rows(pltpu.roll(ext[k, span, pl.ds(base, WIDE)], back, 1)[:, :SIDE], lax.rem(top + RAD, 8))
            for k in range(2)
        ]
        res = jnp.where(own, res, outer[0])
        return jnp.where(res > 0.0, res, FAR), jnp.where(own, mark, outer[1])

    def solve_group(group, _):
        size = jnp.minimum(count - group * PLANES, PLANES)

        def begin(b, _):
            for copy in copies(order[group * PLANES + b], b):
                copy.start()
            return 0

        def ready(b, _):
            b_own = jnp.minimum(b, size - 1)
            slot = order[group * PLANES + b_own]

            @pl.when(b < size)
            def _():
                for copy in copies(slot, b):
                    copy.wait()

            staged[0, b], staged[1, b] = fetch(slot, b_own)
            return 0

        def store(b, cut, current):
            solved[b, cut, :] = current

        def done(b, _):
            top, left = corner_of(centers, order[group * PLANES + b], rows, cols)
            add_window(acc, solved[b], top, left)
            return 0

        lax.fori_loop(0, size, begin, 0)
        lax.fori_loop(0, PLANES, ready, 0)
        solve(lambda b, cut: (staged[0, b, cut, :], staged[1, b, cut, :]), store)
        lax.fori_loop(0, size, done, 0)
        return 0

    lax.fori_loop(0, (count + PLANES - 1) // PLANES, solve_group, 0)

    def place(slot, _):
        top, left = corner_of(centers, slot, rows, cols)

        @pl.when(is_inner(top, left, rows, cols))
        def _():
            add_window(acc, inner_cur[slot], top, left)

        return 0

    lax.fori_loop(0, live[0], place, 0)
    copy = pltpu.make_async_copy(acc.at[pl.ds(RAD, rows), pl.ds(LANES, cols)], out, out_sem)
    copy.start()
    for dr in (-1, 1):
        outs[(dr, 0)][...] = acc[spans[dr][0], spans[0][1]]
    for dr in (-1, 0, 1):
        for dc in (-1, 1):
            tile = acc[spans[dr][0], spans[dc][1]]
            outs[(dr, dc)][...] = pack_high(tile) if dc < 0 else pack_low(tile)
    copy.wait()


def fold_kernel(rows, cols, *refs):
    halos = dict(zip(SHIFTS, refs[1:9]))
    out, upper, lower, left, right, sems = refs[9:]
    last = cols - LANES
    inner_rows = rows - SIDE
    places = (
        (upper, pl.ds(0, RAD), pl.ds(0, cols)),
        (lower, pl.ds(rows - RAD, RAD), pl.ds(0, cols)),
        (left, pl.ds(RAD, inner_rows), pl.ds(0, LANES)),
        (right, pl.ds(RAD, inner_rows), pl.ds(last, LANES)),
    )
    fetch = [pltpu.make_async_copy(out.at[r, c], buf, sems.at[0, k]) for k, (buf, r, c) in enumerate(places)]
    store = [pltpu.make_async_copy(buf, out.at[r, c], sems.at[1, k]) for k, (buf, r, c) in enumerate(places)]
    for copy in fetch:
        copy.start()

    def spread(dr, dc):
        first, second = (to_low if dc < 0 else to_high)(halos[(dr, dc)][...])
        low = lane_ids(first.shape) < RAD
        keep = low if dc < 0 else jnp.logical_not(low)
        return jnp.where(keep, first, 0.0), jnp.where(keep, second, 0.0)

    for copy in fetch:
        copy.wait()
    half = rows // 2
    for dc, buf, at in ((-1, left, 0), (1, right, last)):
        first, second = spread(0, dc)
        buf[0:half - RAD] = buf[0:half - RAD] + first[RAD:]
        buf[half - RAD:inner_rows] = buf[half - RAD:inner_rows] + second[:half - RAD]
        upper[:, at:at + LANES] = upper[:, at:at + LANES] + first[:RAD]
        lower[:, at:at + LANES] = lower[:, at:at + LANES] + second[half - RAD:]
        for dr, strip in ((-1, upper), (1, lower)):
            one, two = spread(dr, dc)
            strip[:RAD // 2, at:at + LANES] = strip[:RAD // 2, at:at + LANES] + one
            strip[RAD // 2:, at:at + LANES] = strip[RAD // 2:, at:at + LANES] + two
    upper[...] = upper[...] + halos[(-1, 0)][...]
    lower[...] = lower[...] + halos[(1, 0)][...]
    for copy in store:
        copy.start()
    for copy in store:
        copy.wait()


def local(resistance, source_mask, target_mask, centers, live_counts):
    rows, cols = resistance.shape
    slots = centers.shape[0]
    f32, i32 = jnp.float32, jnp.int32
    smem = pl.BlockSpec(memory_space=pltpu.SMEM)
    vmem = pl.BlockSpec(memory_space=pltpu.VMEM)
    hbm = pl.BlockSpec(memory_space=pltpu.HBM)

    shapes = {
        at: (RAD if at[0] else rows, cols) if at[1] == 0 else ((RAD if at[0] else rows) // 2, LANES) for at in SHIFTS
    }
    pairs = [pltpu.VMEM((2, *shapes[at]), f32) for at in SHIFTS]
    strips = [pltpu.VMEM(shapes[at], f32) for at in SHIFTS]
    stage = [pltpu.VMEM((2, PLANES, SIDE, SIDE), f32), pltpu.VMEM((PLANES, SIDE, SIDE), f32)]
    kinds = (f32, i32, i32)
    frame_shapes = ((rows, LANES), (rows, LANES), (RAD, cols), (RAD, cols))

    windows = pl.pallas_call(
        functools.partial(cut_kernel, rows, cols),
        out_shape=jax.ShapeDtypeStruct((2, slots, SIDE, SIDE), f32),
        in_specs=[smem, smem, hbm, hbm, hbm],
        out_specs=vmem,
        scratch_shapes=[pltpu.VMEM((slots, TALL, WIDE), kind) for kind in kinds]
        + [pltpu.SemaphoreType.DMA((3, slots))],
        compiler_params=pltpu.CompilerParams(vmem_limit_bytes=57 << 20),
        name="cut",
    )(centers, live_counts, resistance, source_mask, target_mask)

    inner_cur, *halos = pl.pallas_call(
        functools.partial(inner_kernel, rows, cols),
        out_shape=[jax.ShapeDtypeStruct((slots, SIDE, SIDE), f32)]
        + [jax.ShapeDtypeStruct((2, *shapes[at]), f32) for at in SHIFTS],
        in_specs=[vmem, hbm, hbm, hbm],
        out_specs=[vmem] * 9,
        scratch_shapes=pairs
        + pairs
        + [pltpu.VMEM(shape, kind) for shape in frame_shapes for kind in kinds]
        + [pltpu.SemaphoreType.DMA((4, 3)), pltpu.SemaphoreType.DMA((8,)), pltpu.SemaphoreType.DMA((8,))]
        + solver_state(GROUP),
        compiler_params=pltpu.CompilerParams(vmem_limit_bytes=46 << 20, collective_id=0, has_side_effects=True),
        name="inner",
    )(windows, resistance, source_mask, target_mask)

    merged, *currents = pl.pallas_call(
        functools.partial(border_kernel, rows, cols),
        out_shape=[jax.ShapeDtypeStruct((rows, cols), f32)]
        + [jax.ShapeDtypeStruct(shapes[at], f32) for at in SHIFTS],
        in_specs=[smem, smem, vmem, hbm, hbm, hbm] + [vmem] * 8,
        out_specs=[hbm] + [vmem] * 8,
        scratch_shapes=[pltpu.VMEM((PLANES, TALL + SIDE, WIDE), kind) for kind in kinds]
        + [
            pltpu.SemaphoreType.DMA((3, PLANES)),
            pltpu.SMEM((slots,), i32),
            pltpu.VMEM((2, rows + SIDE, cols + WIDE), f32),
            pltpu.VMEM((rows + SIDE, cols + WIDE), f32),
            pltpu.SemaphoreType.DMA,
        ]
        + stage
        + solver_state(PLANES),
        compiler_params=pltpu.CompilerParams(vmem_limit_bytes=42 << 20),
        name="border",
    )(centers, live_counts, inner_cur, resistance, source_mask, target_mask, *halos)

    back = pl.pallas_call(
        return_kernel,
        out_shape=[jax.ShapeDtypeStruct(shapes[at], f32) for at in SHIFTS],
        in_specs=[vmem] * 8,
        out_specs=[vmem] * 8,
        scratch_shapes=strips + [pltpu.SemaphoreType.DMA((8,)), pltpu.SemaphoreType.DMA((8,))],
        compiler_params=pltpu.CompilerParams(vmem_limit_bytes=8 << 20, collective_id=1, has_side_effects=True),
        name="give_back",
    )(*currents)
    out_shape = jax.ShapeDtypeStruct((rows, cols), f32)

    return pl.pallas_call(
        functools.partial(fold_kernel, rows, cols),
        out_shape=out_shape,
        in_specs=[hbm] + [vmem] * 8,
        out_specs=hbm,
        scratch_shapes=[
            pltpu.VMEM((RAD, cols), f32),
            pltpu.VMEM((RAD, cols), f32),
            pltpu.VMEM((rows - SIDE, LANES), f32),
            pltpu.VMEM((rows - SIDE, LANES), f32),
            pltpu.SemaphoreType.DMA((2, 4)),
        ],
        input_output_aliases={0: 0},
        compiler_params=pltpu.CompilerParams(vmem_limit_bytes=16 << 20),
        name="fold",
    )(merged, *back)


def solution(mesh):
    return jax.shard_map(
        local,
        mesh=mesh,
        in_specs=(
            P("row", "col"),
            P("row", "col"),
            P("row", "col"),
            P(("row", "col"), None),
            P(("row", "col")),
        ),
        out_specs=P("row", "col"),
        check_vma=False,
    )
```

```python
import functools

import jax
import jax.numpy as jnp
from jax import lax
from jax.experimental import pallas as pl
from jax.experimental.pallas import tpu as pltpu
from jax.sharding import PartitionSpec as P

RAD = 64
SIDE = 2 * RAD
ITERS = 24
LEAKAGE = 0.02
FAR = 1e37
GROUP = 8
LANES = 128
TALL = SIDE + 8
WIDE = 2 * LANES
SHIFTS = ((0, -1), (0, 1), (-1, 0), (1, 0), (-1, -1), (-1, 1), (1, -1), (1, 1))


def roll(value, shift, axis):
    return pltpu.roll(value, shift % value.shape[axis], axis)


def lane_ids(shape):
    return lax.broadcasted_iota(jnp.int32, shape, 1)


def to_low(packed):
    return packed, roll(packed, RAD, 1)


def to_high(packed):
    return roll(packed, RAD, 1), packed


def pack_low(tile):
    half = tile.shape[0] // 2
    first, second = tile[:half], tile[half:]
    return jnp.where(lane_ids(first.shape) < RAD, first, roll(second, RAD, 1))


def pack_high(tile):
    half = tile.shape[0] // 2
    first, second = tile[:half], tile[half:]
    return jnp.where(lane_ids(first.shape) < RAD, roll(first, RAD, 1), second)


def neighbours():
    row, col = lax.axis_index("row"), lax.axis_index("col")
    rows, cols = lax.axis_size("row"), lax.axis_size("col")
    found = {}
    for (dr, dc) in SHIFTS:
        r, c = row + dr, col + dc
        found[(dr, dc)] = ((r >= 0) & (r < rows) & (c >= 0) & (c < cols), (r, c))
    return found


def greet(found):
    barrier = pltpu.get_barrier_semaphore()
    for at in SHIFTS:
        exists, device = found[at]

        @pl.when(exists)
        def _():
            pl.semaphore_signal(barrier, inc=1, device_id=device, device_id_type=pl.DeviceIdType.MESH)


def all_greeted(found):
    count = sum(found[at][0].astype(jnp.int32) for at in SHIFTS)
    pl.semaphore_wait(pltpu.get_barrier_semaphore(), count)


def transfers(found, pieces, halos, send_sems, recv_sems, ats=SHIFTS):
    made = []
    for at in ats:
        k = SHIFTS.index(at)
        exists, device = found[at]
        back = (-at[0], -at[1])
        made.append((exists, pltpu.make_async_remote_copy(
            src_ref=pieces[at],
            dst_ref=halos[back],
            send_sem=send_sems.at[k],
            recv_sem=recv_sems.at[SHIFTS.index(back)],
            device_id=device,
            device_id_type=pl.DeviceIdType.MESH,
        )))
    return made


def landings(found, pieces, halos, send_sems, recv_sems, ats=SHIFTS):
    made = []
    for at in ats:
        k = SHIFTS.index(at)
        exists, device = found[at]
        made.append((exists, pltpu.make_async_remote_copy(
            src_ref=pieces[at],
            dst_ref=halos[at],
            send_sem=send_sems.at[k],
            recv_sem=recv_sems.at[k],
            device_id=device,
            device_id_type=pl.DeviceIdType.MESH,
        )))
    return made


def start_all(copies):
    for exists, copy in copies:
        pl.when(exists)(copy.start)


def finish_all(copies, arrivals):
    for exists, copy in copies:
        pl.when(exists)(copy.wait_send)
    for exists, copy in arrivals:
        pl.when(exists)(copy.wait_recv)


def corner_of(centers, slot, rows, cols):
    return lax.rem(centers[0, slot], rows) - RAD, lax.rem(centers[1, slot], cols) - RAD


def is_inner(top, left, rows, cols):
    return (top >= 0) & (top <= rows - SIDE) & (left >= 0) & (left <= cols - SIDE)


def clamped(top, left, rows, cols):
    row = jnp.clip((top + RAD) // 8 * 8 - RAD, 0, rows - TALL)
    col = jnp.clip((left + LANES) // LANES * LANES - LANES, 0, cols - WIDE)
    return pl.multiple_of(row, 8), pl.multiple_of(col, LANES)


def total(values):
    return jnp.sum(jnp.sum(values, axis=0, keepdims=True), axis=1, keepdims=True)


def cut_rows(value, skip):
    return pltpu.roll(value, lax.rem(TALL - skip, TALL), 0)[:SIDE]


def add_window(acc, current, top, left):
    col = pl.multiple_of((left + LANES) // LANES * LANES, LANES)
    shift = left + LANES - col
    wide = jnp.concatenate([current, jnp.zeros_like(current)], axis=1)
    wide = pltpu.roll(wide, shift, 1)
    wide = jnp.concatenate([wide, jnp.zeros((8, WIDE), jnp.float32)], axis=0)
    wide = pltpu.roll(wide, lax.rem(top + RAD, 8), 0)
    rows = pl.ds(pl.multiple_of((top + RAD) // 8 * 8, 8), TALL)
    acc[rows, pl.ds(col, WIDE)] = acc[rows, pl.ds(col, WIDE)] + wide


PLANES = 4
CHUNK = 64
SEGMENTS = SIDE // PLANES
EIGHTS = tuple(slice(8 * k, 8 * k + 8) for k in range(SIDE // 8))


def lanes_of(shape):
    return lax.broadcasted_iota(jnp.int32, shape, 1)


def interleave(shape, transposed):
    row, col = (lax.broadcasted_iota(jnp.int32, shape, axis) for axis in (0, 1))
    if transposed:
        row, col = col, row
    window, place = row // SIDE, row % SIDE
    return (col == (place % PLANES) * SIDE + window * SEGMENTS + place // PLANES).astype(jnp.bfloat16)


def halves(value):
    high = value.astype(jnp.bfloat16)
    return high, (value - high.astype(jnp.float32)).astype(jnp.bfloat16)


def mixed(parts, table):
    found = jnp.dot(jnp.concatenate(parts, axis=0), table[...], preferred_element_type=jnp.float32)
    size = parts[0].shape[0]
    return [found[size * n:size * n + size] for n in range(len(parts))]


def quad_state():
    f32 = jnp.float32
    planes = pltpu.VMEM((PLANES, SIDE, SIDE), f32)
    padded = pltpu.VMEM((PLANES, SIDE + 16, SIDE), f32)
    tile = pltpu.VMEM((SIDE, SIDE), f32)
    table = pltpu.VMEM((ITERS, 8, SIDE), f32)
    return (
        [padded, padded, pltpu.VMEM((ITERS, PLANES, SIDE, SIDE), f32), planes]
        + [padded, planes, tile]
        + [tile, tile]
        + [padded, planes, planes, padded, padded, planes]
        + [table, table]
    )


def solver_state(group):
    wide = PLANES * SIDE
    return quad_state() * (group // PLANES) + [pltpu.VMEM((2, wide, wide), jnp.bfloat16)]


def quad_parts(state):
    even, odd, hist, t_s, vert, hori, hori_in, edge_r, edge_l, isd_s, inj_s, gnd_s, v_s, res_s, h_s, tail_s, link_s = state
    f32 = jnp.float32
    mid = tuple(slice(8 + 8 * k, 16 + 8 * k) for k in range(SIDE // 8))
    low = tuple(slice(9 + 8 * k, 17 + 8 * k) for k in range(SIDE // 8))
    upp = tuple(slice(7 + 8 * k, 15 + 8 * k) for k in range(SIDE // 8))
    blocks = range(SIDE // 8)
    lane = lanes_of((8, SIDE))
    row8 = lax.broadcasted_iota(jnp.int32, (8, SIDE), 0)

    def clear():
        zero = jnp.zeros((8, SIDE), f32)
        for pad in (even, odd, vert, isd_s, v_s, res_s):
            for p in range(PLANES):
                pad[p, 0:8, :] = zero
                pad[p, 8 + SIDE:16 + SIDE, :] = zero

    def refresh_edges(cur):
        for k in blocks:
            edge_r[EIGHTS[k], :] = roll(cur[0, mid[k], :], -1, 1)
            edge_l[EIGHTS[k], :] = roll(cur[PLANES - 1, mid[k], :], 1, 1)

    def operate(cur):
        gammas, deltas = [None] * PLANES, [None] * PLANES
        for k in blocks:
            here = [cur[p, mid[k], :] for p in range(PLANES)]
            out = [hori[p, EIGHTS[k], :] for p in range(PLANES)]
            for p in (1, 2, 0, 3):
                right = here[p + 1] if p < PLANES - 1 else edge_r[EIGHTS[k], :]
                left = here[p - 1] if p else edge_l[EIGHTS[k], :]
                back = out[p - 1] if p else hori_in[EIGHTS[k], :]
                beside = vert[p, mid[k], :] * cur[p, low[k], :] + vert[p, upp[k], :] * cur[p, upp[k], :]
                beside = beside + (out[p] * right + back * left)
                t_s[p, EIGHTS[k], :] = beside
                one, two = here[p] * here[p], here[p] * beside
                gammas[p] = one if k == 0 else gammas[p] + one
                deltas[p] = two if k == 0 else deltas[p] + two
        return (gammas[0] + gammas[1]) + (gammas[2] + gammas[3]), (deltas[0] + deltas[1]) + (deltas[2] + deltas[3])

    def down_sum(part):
        for shift in (4, 2, 1):
            part = part + roll(part, shift, 0)
        return part

    def total_of(sums):
        mine = lane // SEGMENTS == row8 % PLANES
        first = row8 < PLANES
        both = jnp.where(first, down_sum(sums[0]), down_sum(sums[1]))
        both = jnp.where(mine, jnp.sum(jnp.where(mine, both, 0.0), axis=1, keepdims=True), 0.0)
        return down_sum(jnp.where(first, both, 0.0)), down_sum(jnp.where(first, 0.0, both))

    def prepare(load, table):
        for r in range(0, SIDE, CHUNK):
            cut = slice(r, r + CHUNK)
            loaded = [load(w, cut) for w in range(PLANES)]
            res = jnp.concatenate([pair[0] for pair in loaded], axis=1)
            mark = jnp.concatenate([pair[1] for pair in loaded], axis=1)
            high, low_part, mark = mixed([*halves(res), mark.astype(jnp.bfloat16)], table)
            res = high + low_part
            signed = mark / res
            for p in range(PLANES):
                span = slice(SIDE * p, SIDE * p + SIDE)
                res_s[p, 8 + r:8 + r + CHUNK, :] = res[:, span]
                inject = jnp.maximum(signed[:, span], 0.0)
                if p == 0 and r <= RAD < r + CHUNK:
                    at = lax.broadcasted_iota(jnp.int32, (CHUNK, SIDE), 0) == RAD - r
                    spot = lanes_of((CHUNK, SIDE)) % SEGMENTS == RAD // PLANES
                    inject = inject + (at & spot).astype(f32)
                inj_s[p, cut, :] = inject
                gnd_s[p, cut, :] = jnp.maximum(-signed[:, span], 0.0)
        ends = lane % SEGMENTS == SEGMENTS - 1
        bottom = row8 == 7
        for k in blocks:
            for p in range(PLANES):
                here = res_s[p, mid[k], :]
                under = res_s[p, low[k], :]
                if k == len(EIGHTS) - 1:
                    vertical = jnp.where(bottom, 0.0, 2.0 / (here + jnp.where(bottom, FAR, under)))
                else:
                    vertical = 2.0 / (here + under)
                v_s[p, mid[k], :] = vertical
                if p < PLANES - 1:
                    h_s[p, EIGHTS[k], :] = 2.0 / (here + res_s[p + 1, mid[k], :])
                else:
                    horizontal = jnp.where(ends, 0.0, 2.0 / (here + roll(res_s[0, mid[k], :], -1, 1)))
                    h_s[p, EIGHTS[k], :] = horizontal
                    edge_l[EIGHTS[k], :] = roll(horizontal, 1, 1)
        for k in blocks:
            for p in range(PLANES):
                before = h_s[p - 1, EIGHTS[k], :] if p else edge_l[EIGHTS[k], :]
                diagonal = v_s[p, mid[k], :] + v_s[p, upp[k], :] + (h_s[p, EIGHTS[k], :] + before)
                isd_s[p, mid[k], :] = 1.0 / jnp.sqrt(diagonal + gnd_s[p, EIGHTS[k], :] + LEAKAGE)
        for k in blocks:
            for p in range(PLANES):
                isd = isd_s[p, mid[k], :]
                vert[p, mid[k], :] = v_s[p, mid[k], :] * isd * isd_s[p, low[k], :]
                if p < PLANES - 1:
                    hori[p, EIGHTS[k], :] = h_s[p, EIGHTS[k], :] * isd * isd_s[p + 1, mid[k], :]
                else:
                    scaled = h_s[p, EIGHTS[k], :] * isd * roll(isd_s[0, mid[k], :], -1, 1)
                    hori[p, EIGHTS[k], :] = scaled
                    hori_in[EIGHTS[k], :] = roll(scaled, 1, 1)
                first = inj_s[p, EIGHTS[k], :] * isd
                even[p, mid[k], :] = first
                hist[0, p, EIGHTS[k], :] = first
        refresh_edges(even)
        return operate(even)

    def settle(j, sums, gamma_inv_before, pivot_inv, weight):
        gamma, delta = sums
        gamma_inv = 1.0 / gamma
        mean = delta * gamma_inv
        ratio = gamma * gamma_inv_before
        link = ratio * pivot_inv
        pivot_inv = 1.0 / (1.0 - mean - link)
        weight = weight * pivot_inv
        tail_s[j] = weight
        link_s[j] = link
        return mean, ratio, gamma_inv, pivot_inv, weight

    def update(j, way, mean, ratio):
        cur, new = (odd, even) if way else (even, odd)
        for p in (0, 3, 1, 2):
            for k in blocks:
                fresh = t_s[p, EIGHTS[k], :] - mean * cur[p, mid[k], :]
                if ratio is not None:
                    fresh = fresh - ratio * new[p, mid[k], :]
                new[p, mid[k], :] = fresh
                hist[j + 1, p, EIGHTS[k], :] = fresh
                if p == 0:
                    edge_r[EIGHTS[k], :] = roll(fresh, -1, 1)
                if p == PLANES - 1:
                    edge_l[EIGHTS[k], :] = roll(fresh, 1, 1)
        return operate(new)

    def coefficients():
        factor = tail_s[ITERS - 1]
        for j in reversed(range(1, ITERS)):
            ahead = tail_s[j - 1] + link_s[j] * factor
            tail_s[j] = factor
            factor = ahead
        tail_s[0] = factor

    def voltages():
        def one(p, _):
            for half in range(2):
                found = [None] * 8
                for j in range(ITERS):
                    factor = tail_s[j]
                    for i in range(8):
                        term = factor * hist[j, p, EIGHTS[8 * half + i], :]
                        found[i] = term if found[i] is None else found[i] + term
                for i in range(8):
                    even[p, mid[8 * half + i], :] = found[i] * isd_s[p, mid[8 * half + i], :]
            return 0

        lax.fori_loop(0, PLANES, one, 0)

    def finish(put, table):
        cur = even
        for k in blocks:
            edge_r[EIGHTS[k], :] = roll(cur[0, mid[k], :], -1, 1)
        for k in blocks:
            for p in range(PLANES):
                volts = cur[p, mid[k], :]
                res_s[p, mid[k], :] = v_s[p, mid[k], :] * jnp.abs(volts - cur[p, low[k], :])
                right = cur[p + 1, mid[k], :] if p < PLANES - 1 else edge_r[EIGHTS[k], :]
                flow = h_s[p, EIGHTS[k], :] * jnp.abs(volts - right)
                t_s[p, EIGHTS[k], :] = flow
                if p == PLANES - 1:
                    edge_l[EIGHTS[k], :] = roll(flow, 1, 1)

        for r in range(0, SIDE, CHUNK):
            cut = slice(r, r + CHUNK)
            pieces = []
            for p in range(PLANES):
                flow = res_s[p, 8 + r:8 + r + CHUNK, :] + res_s[p, 7 + r:7 + r + CHUNK, :] + t_s[p, cut, :]
                flow = flow + (t_s[p - 1, cut, :] if p else edge_l[cut, :])
                pieces.append(0.5 * (flow + inj_s[p, cut, :] + gnd_s[p, cut, :] * jnp.abs(cur[p, 8 + r:8 + r + CHUNK, :])))
            high, low_part = mixed(halves(jnp.concatenate(pieces, axis=1)), table)
            for w in range(PLANES):
                span = slice(SIDE * w, SIDE * w + SIDE)
                put(w, cut, high[:, span] + low_part[:, span])

    return clear, prepare, total_of, operate, settle, update, coefficients, voltages, finish


def solver_parts(state, group):
    table = state[-1]
    count = group // PLANES
    size = (len(state) - 1) // count
    quads = [quad_parts(state[size * q:size * q + size]) for q in range(count)]

    def clear():
        for quad in quads:
            quad[0]()
        for way in range(2):
            table[way] = interleave(table.shape[1:], way == 1)

    def solve(load, store):
        one = jnp.ones((8, SIDE), jnp.float32)
        carry = []
        for q, (_, prepare, total_of, *_) in enumerate(quads):
            sums = prepare(lambda w, cut, q=q: load(PLANES * q + w, cut), table.at[0])
            carry.append((sums if q else total_of(sums), 0.0 * one, 0.0 * one, one))

        def step(j, way, carry, first=False):
            after = []
            for q, (_, _, total_of, operate, settle, update, *_) in enumerate(quads):
                sums, *rest = carry[q]
                if q:
                    sums = total_of(sums)
                mean, ratio, *rest = settle(j, sums, *rest)
                sums = update(j, way, mean, None if first else ratio)
                after.append((sums if q else total_of(sums), *rest))
            return after

        def steps(i, carry):
            return tuple(step(2 * i + 2, 0, step(2 * i + 1, 1, carry)))

        carry = tuple(step(0, 0, carry, True))
        carry = lax.fori_loop(0, (ITERS - 2) // 2, steps, carry)
        for q, (_, _, total_of, _, settle, _, coefficients, *_) in enumerate(quads):
            settle(ITERS - 1, total_of(carry[q][0]) if q else carry[q][0], *carry[q][1:])
            coefficients()
        for q, (*_, voltages, finish) in enumerate(quads):
            voltages()
            finish(lambda w, cut, tile, q=q: store(PLANES * q + w, cut, tile), table.at[1])

    return clear, solve


def spans_of(rows, cols):
    return {
        -1: (slice(0, RAD), slice(0, LANES)),
        0: (slice(RAD, RAD + rows), slice(LANES, LANES + cols)),
        1: (slice(RAD + rows, SIDE + rows), slice(LANES + cols, WIDE + cols)),
    }


def mark_of(source, target):
    source, target = source.astype(jnp.float32), target.astype(jnp.float32)
    return source - target * (1.0 - source)


def turn_own(res, source, target, skip, turn):
    source, target = source.astype(jnp.float32), target.astype(jnp.float32)
    mark = source - target * (1.0 - source)
    turn = lax.rem(WIDE + turn, WIDE)
    res = cut_rows(pltpu.roll(res, turn, 1)[:, :SIDE], skip)
    mark = cut_rows(pltpu.roll(mark, turn, 1)[:, :SIDE], skip)
    return res, mark


def strips_kernel(rows, cols, *refs):
    raw = refs[:3]
    outs = dict(zip(SHIFTS, refs[3:11]))
    pieces, halos = dict(zip(SHIFTS, refs[11:19])), dict(zip(SHIFTS, refs[19:27]))
    frames = [refs[27 + 3 * k:30 + 3 * k] for k in range(4)]
    sems, send_sems, recv_sems = refs[39:42]
    found = neighbours()

    everything = pl.ds(0, rows)
    places = (
        (everything, pl.ds(0, LANES)),
        (everything, pl.ds(cols - LANES, LANES)),
        (pl.ds(0, RAD), pl.ds(0, cols)),
        (pl.ds(rows - RAD, RAD), pl.ds(0, cols)),
    )
    frame_copies = [
        [pltpu.make_async_copy(raw[k].at[places[f]], frames[f][k], sems.at[f, k]) for k in range(3)]
        for f in range(4)
    ]
    for copy in sum(frame_copies, []):
        copy.start()
    for at in SHIFTS:
        halos[at][...] = jnp.zeros_like(halos[at])
    greet(found)

    def strengths(frame, cut=slice(None)):
        res, source, target = (ref[cut] for ref in frame)
        source, target = source.astype(jnp.float32), target.astype(jnp.float32)
        return res, source - target * (1.0 - source)

    for f, at in enumerate(((0, -1), (0, 1), (-1, 0), (1, 0))):
        for copy in frame_copies[f]:
            copy.wait()
        for k, value in enumerate(strengths(frames[f])):
            if at[1] == 0:
                pieces[at][k] = value
            else:
                squeeze = pack_low if at[1] < 0 else pack_high
                pieces[at][k] = squeeze(value)
                pieces[(-1, at[1])][k] = squeeze(value[:RAD])
                pieces[(1, at[1])][k] = squeeze(value[rows - RAD:])
    all_greeted(found)
    copies = transfers(found, pieces, halos, send_sems, recv_sems)
    start_all(copies)

    finish_all(copies, landings(found, pieces, halos, send_sems, recv_sems))
    for at in SHIFTS:
        outs[at][...] = halos[at][...]


def return_kernel(*refs):
    pieces, outs, halos = (dict(zip(SHIFTS, refs[8 * k:8 * k + 8])) for k in range(3))
    send_sems, recv_sems = refs[24:]
    found = neighbours()
    for at in SHIFTS:
        halos[at][...] = jnp.zeros_like(halos[at])
    greet(found)
    all_greeted(found)
    copies = transfers(found, pieces, halos, send_sems, recv_sems)
    start_all(copies)
    finish_all(copies, landings(found, pieces, halos, send_sems, recv_sems))
    for at in SHIFTS:
        outs[at][...] = halos[at][...]


def border_kernel(rows, cols, centers, live, *refs):
    raw, halos = refs[:3], dict(zip(SHIFTS, refs[3:11]))
    out, outs = refs[11], dict(zip(SHIFTS, refs[12:20]))
    bufs, sems, ext, acc, out_sem, staged, solved = refs[20:23], *refs[23:29]
    clear, solve = solver_parts(refs[29:], PLANES)

    def copies(slot, at):
        top, left = corner_of(centers, slot, rows, cols)
        row, col = clamped(top, left, rows, cols)
        return [
            pltpu.make_async_copy(
                src.at[pl.ds(row, TALL), pl.ds(col, WIDE)],
                dst.at[at, pl.ds(RAD, TALL), :],
                sems.at[k, at],
            )
            for k, (src, dst) in enumerate(zip(raw, bufs))
        ]

    count = live[0]
    acc[...] = jnp.zeros_like(acc)
    clear()
    spans = spans_of(rows, cols)
    for which in range(2):
        for dr in (-1, 1):
            ext[which, spans[dr][0], spans[0][1]] = halos[(dr, 0)][which]
        for dr in (-1, 0, 1):
            start, stop = spans[dr][0].start, spans[dr][0].stop
            middle = (start + stop) // 2
            for dc in (-1, 1):
                split = to_high if dc < 0 else to_low
                first, second = split(halos[(dr, dc)][which])
                ext[which, start:middle, spans[dc][1]] = first
                ext[which, middle:stop, spans[dc][1]] = second

    row_id = lax.broadcasted_iota(jnp.int32, (SIDE, SIDE), 0)
    col_id = lax.broadcasted_iota(jnp.int32, (SIDE, SIDE), 1)

    def fetch(slot, b):
        top, left = corner_of(centers, slot, rows, cols)
        row, col = clamped(top, left, rows, cols)
        take = pl.ds(pl.multiple_of((RAD + top - row) // 8 * 8, 8), TALL)
        res, source, target = (buf[b, take, :] for buf in bufs)
        res, mark = turn_own(res, source, target, lax.rem(RAD + top - row, 8), col - left)
        at_row, at_col = row_id + top, col_id + left
        own = (at_row >= 0) & (at_row < rows) & (at_col >= 0) & (at_col < cols)
        base = pl.multiple_of((left + LANES) // LANES * LANES, LANES)
        back = lax.rem(WIDE + base - left - LANES, WIDE)
        span = pl.ds(pl.multiple_of((top + RAD) // 8 * 8, 8), TALL)
        outer = [
            cut_rows(pltpu.roll(ext[k, span, pl.ds(base, WIDE)], back, 1)[:, :SIDE], lax.rem(top + RAD, 8))
            for k in range(2)
        ]
        res = jnp.where(own, res, outer[0])
        return jnp.where(res > 0.0, res, FAR), jnp.where(own, mark, outer[1])

    def solve_group(group, _):
        size = jnp.minimum(count - group * PLANES, PLANES)

        def begin(b, _):
            for copy in copies((group * PLANES + b), b):
                copy.start()
            return 0

        def ready(b, _):
            b_own = jnp.minimum(b, size - 1)
            slot = (group * PLANES + b_own)

            @pl.when(b < size)
            def _():
                for copy in copies(slot, b):
                    copy.wait()

            staged[0, b], staged[1, b] = fetch(slot, b_own)
            return 0

        def store(b, cut, current):
            solved[b, cut, :] = current

        def done(b, _):
            top, left = corner_of(centers, (group * PLANES + b), rows, cols)
            add_window(acc, solved[b], top, left)
            return 0

        lax.fori_loop(0, size, begin, 0)
        lax.fori_loop(0, PLANES, ready, 0)
        solve(lambda b, cut: (staged[0, b, cut, :], staged[1, b, cut, :]), store)
        lax.fori_loop(0, size, done, 0)
        return 0

    lax.fori_loop(0, (count + PLANES - 1) // PLANES, solve_group, 0)

    copy = pltpu.make_async_copy(acc.at[pl.ds(RAD, rows), pl.ds(LANES, cols)], out, out_sem)
    copy.start()
    for dr in (-1, 1):
        outs[(dr, 0)][...] = acc[spans[dr][0], spans[0][1]]
    for dr in (-1, 0, 1):
        for dc in (-1, 1):
            tile = acc[spans[dr][0], spans[dc][1]]
            outs[(dr, dc)][...] = pack_high(tile) if dc < 0 else pack_low(tile)
    copy.wait()


def fold_kernel(rows, cols, *refs):
    halos = dict(zip(SHIFTS, refs[1:9]))
    out, upper, lower, left, right, sems = refs[9:]
    last = cols - LANES
    inner_rows = rows - SIDE
    places = (
        (upper, pl.ds(0, RAD), pl.ds(0, cols)),
        (lower, pl.ds(rows - RAD, RAD), pl.ds(0, cols)),
        (left, pl.ds(RAD, inner_rows), pl.ds(0, LANES)),
        (right, pl.ds(RAD, inner_rows), pl.ds(last, LANES)),
    )
    fetch = [pltpu.make_async_copy(out.at[r, c], buf, sems.at[0, k]) for k, (buf, r, c) in enumerate(places)]
    store = [pltpu.make_async_copy(buf, out.at[r, c], sems.at[1, k]) for k, (buf, r, c) in enumerate(places)]
    for copy in fetch:
        copy.start()

    def spread(dr, dc):
        first, second = (to_low if dc < 0 else to_high)(halos[(dr, dc)][...])
        low = lane_ids(first.shape) < RAD
        keep = low if dc < 0 else jnp.logical_not(low)
        return jnp.where(keep, first, 0.0), jnp.where(keep, second, 0.0)

    for copy in fetch:
        copy.wait()
    half = rows // 2
    for dc, buf, at in ((-1, left, 0), (1, right, last)):
        first, second = spread(0, dc)
        buf[0:half - RAD] = buf[0:half - RAD] + first[RAD:]
        buf[half - RAD:inner_rows] = buf[half - RAD:inner_rows] + second[:half - RAD]
        upper[:, at:at + LANES] = upper[:, at:at + LANES] + first[:RAD]
        lower[:, at:at + LANES] = lower[:, at:at + LANES] + second[half - RAD:]
        for dr, strip in ((-1, upper), (1, lower)):
            one, two = spread(dr, dc)
            strip[:RAD // 2, at:at + LANES] = strip[:RAD // 2, at:at + LANES] + one
            strip[RAD // 2:, at:at + LANES] = strip[RAD // 2:, at:at + LANES] + two
    upper[...] = upper[...] + halos[(-1, 0)][...]
    lower[...] = lower[...] + halos[(1, 0)][...]
    for copy in store:
        copy.start()
    for copy in store:
        copy.wait()


MAIN = SHIFTS[:4]
PIECES = 4


def wait_for(found, ats, peers):
    count = sum(found[at][0].astype(jnp.int32) for at in ats) + len(peers)
    pl.semaphore_wait(pltpu.get_barrier_semaphore(), count)


def hello(found, ats, peers):
    barrier = pltpu.get_barrier_semaphore()
    for at in ats:
        exists, device = found[at]

        @pl.when(exists)
        def _():
            pl.semaphore_signal(barrier, inc=1, device_id=device, device_id_type=pl.DeviceIdType.MESH)

    for device in peers:
        pl.semaphore_signal(barrier, inc=1, device_id=device, device_id_type=pl.DeviceIdType.MESH)


def peers_along(axis):
    row, col = lax.axis_index("row"), lax.axis_index("col")
    size = lax.axis_size(axis)
    if axis == "row":
        return [(lax.rem(row + k, size), col) for k in range(1, size)]
    return [(row, lax.rem(col + k, size)) for k in range(1, size)]


def share_flag(flag, landed, peers, send_sems, recv_sems):
    return [
        pltpu.make_async_remote_copy(
            src_ref=flag, dst_ref=landed.at[k], send_sem=send_sems.at[k], recv_sem=recv_sems.at[k],
            device_id=device, device_id_type=pl.DeviceIdType.MESH,
        )
        for k, device in enumerate(peers)
    ]


def largest(flag, landed, peers):
    found = flag[...]
    for k in range(len(peers)):
        found = jnp.maximum(found, landed[k])
    return found


def meta_kernel(centers, live, out, mine, halos, send_sems, recv_sems):
    found = neighbours()
    halos[...] = jnp.zeros_like(halos)
    hello(found, MAIN, [])
    slots = centers.shape[1]
    row8 = lax.broadcasted_iota(jnp.int32, (8, LANES), 0)
    lane8 = lanes_of((8, LANES))
    block = jnp.broadcast_to(live[0], (8, LANES)).astype(jnp.int32)
    for s in range(slots):
        for axis in range(2):
            block = jnp.where((row8 == axis) & (lane8 == s), centers[axis, s], block)
    mine[...] = block
    wait_for(found, MAIN, [])
    args = (found, {at: mine for at in MAIN}, {at: halos.at[k] for k, at in enumerate(MAIN)}, send_sems, recv_sems)
    copies = transfers(*args, ats=MAIN)
    start_all(copies)
    finish_all(copies, landings(*args, ats=MAIN))
    out[...] = halos[...]


def crosses(at, top, left, rows, cols):
    tests = {(0, -1): left < 0, (0, 1): left + SIDE > cols, (-1, 0): top < 0, (1, 0): top + SIDE > rows}
    return tests[at]


def spot_of(at, row_of, col_of, slot, rows, cols):
    return lax.rem(row_of(slot), rows) - RAD, lax.rem(col_of(slot), cols) - RAD


def pack_kernel(rows, cols, centers, live, meta, *refs):
    raw, windows, order = refs[:3], refs[3], refs[4]
    pieces, flag = dict(zip(SHIFTS, refs[5:13])), refs[13]
    bufs, piece_bufs, corner_bufs, sems, piece_sems, corner_sems = refs[14:17], refs[17:20], refs[20:23], *refs[23:26]
    slots = centers.shape[1]
    found = neighbours()

    def corner(slot):
        return lax.rem(centers[0, slot], rows) - RAD, lax.rem(centers[1, slot], cols) - RAD

    def place(slot):
        top, left = corner(slot)
        return top, left, *clamped(top, left, rows, cols)

    def copies(slot):
        _, _, row, col = place(slot)
        return [
            pltpu.make_async_copy(src.at[pl.ds(row, TALL), pl.ds(col, WIDE)], dst.at[slot], sems.at[k, slot])
            for k, (src, dst) in enumerate(zip(raw, bufs))
        ]

    def classify(slot, carry):
        inner, outer, crossing = carry
        for copy in copies(slot):
            copy.start()
        top, left = corner(slot)
        inside = is_inner(top, left, rows, cols)
        at = jnp.where(inside, inner, slots - 1 - outer)
        order[0, at] = slot
        step = inside.astype(jnp.int32)
        fresh = []
        for d, way in enumerate(MAIN):
            over = crosses(way, top, left, rows, cols) & found[way][0]
            order[2 + d, slot] = jnp.minimum(crossing[d], PIECES - 1)
            fresh.append(crossing[d] + over.astype(jnp.int32))
        return inner + step, outer + 1 - step, tuple(fresh)

    zero = jnp.int32(0)
    inner, outer, crossing = lax.fori_loop(0, live[0], classify, (zero, zero, (zero,) * 4))
    order[1, 0] = inner
    most = jnp.maximum(jnp.maximum(crossing[0], crossing[1]), jnp.maximum(crossing[2], crossing[3]))
    flag[...] = jnp.broadcast_to((most > PIECES).astype(jnp.int32), flag.shape)

    corners = []
    for n, at in enumerate(SHIFTS[4:]):
        r = pl.ds(0 if at[0] < 0 else rows - RAD, RAD)
        c = pl.ds(0 if at[1] < 0 else cols - LANES, LANES)
        corners += [
            pltpu.make_async_copy(src.at[r, c], dst.at[n], corner_sems.at[k, n])
            for k, (src, dst) in enumerate(zip(raw, corner_bufs))
        ]
    for copy in corners:
        copy.start()

    def theirs(d, slot):
        return lax.rem(meta[d, 0, slot], rows) - RAD, lax.rem(meta[d, 1, slot], cols) - RAD

    def piece_place(d, k):
        at = MAIN[d]
        top, left = theirs(d, order[6 + d, k])
        if at[1]:
            row = pl.multiple_of(jnp.clip((top + RAD) // 8 * 8 - RAD, 0, rows - TALL), 8)
            return row, 0 if at[1] < 0 else cols - LANES, top - row
        col = pl.multiple_of(jnp.clip((left + LANES) // LANES * LANES - LANES, 0, cols - WIDE), LANES)
        return 0 if at[0] < 0 else rows - RAD, col, left - col

    def piece_copies(d, k):
        row, col, _ = piece_place(d, k)
        size = (TALL, LANES) if MAIN[d][1] else (RAD, WIDE)
        return [
            pltpu.make_async_copy(
                src.at[pl.ds(row, size[0]), pl.ds(col, size[1])],
                dst.at[d, k, pl.ds(0, size[0]), pl.ds(0, size[1])],
                piece_sems.at[n, d, k],
            )
            for n, (src, dst) in enumerate(zip(raw, piece_bufs))
        ]

    counts = []
    for d, at in enumerate(MAIN):
        back = (-at[0], -at[1])

        def look(slot, count, d=d, back=back):
            top, left = theirs(d, slot)
            hit = crosses(back, top, left, rows, cols)

            @pl.when(hit & (count < PIECES))
            def _():
                order[6 + d, count] = slot
                for copy in piece_copies(d, count):
                    copy.start()

            return count + hit.astype(jnp.int32)

        limit = jnp.where(found[at][0], meta[d, 2, 0], 0)
        count = jnp.minimum(lax.fori_loop(0, limit, look, zero), PIECES)
        order[1, 1 + d] = count
        counts.append(count)

    def blank(slot, _):
        windows[0, slot] = jnp.ones((SIDE, SIDE), jnp.float32)
        windows[1, slot] = jnp.zeros((SIDE, SIDE), jnp.float32)
        return 0

    def cut(n, _):
        at = jnp.where(n < inner, n, slots - 1 - (n - inner))
        slot = order[0, at]
        for copy in copies(slot):
            copy.wait()
        top, left, row, col = place(slot)
        res, mark = turn_own(*(buf[slot] for buf in bufs), top - row, col - left)
        windows[0, at] = res
        windows[1, at] = mark
        return 0

    lax.fori_loop(inner, slots - outer, blank, 0)
    lax.fori_loop(0, live[0], cut, 0)
    for n, at in enumerate(SHIFTS[4:]):
        for k in range(3):
            corners[3 * n + k].wait()
        squeeze = pack_low if at[1] < 0 else pack_high
        res, source, target = (buf[n] for buf in corner_bufs)
        pieces[at][0] = squeeze(res)
        pieces[at][1] = squeeze(mark_of(source, target))
    for d, at in enumerate(MAIN):
        def fill(k, _, d=d, at=at):
            for copy in piece_copies(d, k):
                copy.wait()
            _, _, skip = piece_place(d, k)
            if at[1]:
                res, source, target = (buf[d, k, :, 0:LANES] for buf in piece_bufs)
                squeeze = pack_low if at[1] < 0 else pack_high
                pieces[at][0, k] = squeeze(cut_rows(res, skip))
                pieces[at][1, k] = squeeze(cut_rows(mark_of(source, target), skip))
            else:
                res, source, target = (buf[d, k, 0:RAD, :] for buf in piece_bufs)
                turn = lax.rem(2 * WIDE - skip, WIDE)
                pieces[at][0, k] = pltpu.roll(res, turn, 1)[:, :SIDE]
                pieces[at][1, k] = pltpu.roll(mark_of(source, target), turn, 1)[:, :SIDE]
            return 0

        lax.fori_loop(0, counts[d], fill, 0)


def trade_kernel(windows, flag, *refs):
    pieces = dict(zip(SHIFTS, refs[:8]))
    cur, outs, flag_out = refs[8], dict(zip(SHIFTS, refs[9:17])), refs[17]
    halos = dict(zip(SHIFTS, refs[18:26]))
    flag_landed, send_sems, recv_sems, flag_send, flag_recv = refs[26:31]
    clear, solve = solver_parts(refs[31:], GROUP)
    found = neighbours()
    peers = peers_along("row")
    for at in SHIFTS:
        halos[at][...] = jnp.zeros_like(halos[at])
    hello(found, SHIFTS, peers)
    wait_for(found, SHIFTS, peers)
    copies = transfers(found, pieces, halos, send_sems, recv_sems)
    start_all(copies)
    shared = share_flag(flag, flag_landed, peers, flag_send, flag_recv)
    for copy in shared:
        copy.start()
    clear()

    def store(b, cut, current):
        cur[b, cut, :] = current

    solve(lambda b, cut: (windows[0, b, cut, :], windows[1, b, cut, :]), store)
    for copy in shared:
        copy.wait()
    flag_out[...] = largest(flag, flag_landed, peers)
    finish_all(copies, landings(found, pieces, halos, send_sems, recv_sems))
    for at in SHIFTS:
        outs[at][...] = halos[at][...]


def unpacked(packed, dc):
    return jnp.concatenate((to_high if dc < 0 else to_low)(packed), axis=0)


def rest_kernel(rows, cols, centers, live, order, windows, inner_cur, *refs):
    halos, out, outs = dict(zip(SHIFTS, refs[:8])), refs[8], dict(zip(SHIFTS, refs[9:17]))
    acc, out_sem, staged, solved = refs[17:21]
    clear, solve = solver_parts(refs[21:], GROUP)
    slots = centers.shape[1]
    inner = order[1, 0]
    ready_count = jnp.minimum(inner, GROUP)
    acc[...] = jnp.zeros_like(acc)
    clear()
    row_id = lax.broadcasted_iota(jnp.int32, (SIDE, SIDE), 0)
    col_id = lax.broadcasted_iota(jnp.int32, (SIDE, SIDE), 1)
    blank = jnp.zeros((RAD, SIDE), jnp.float32)

    def corner(slot):
        return lax.rem(centers[0, slot], rows) - RAD, lax.rem(centers[1, slot], cols) - RAD

    def seat(n):
        return jnp.where(n < inner, n, slots - 1 - (n - inner))

    def place(n, _):
        top, left = corner(order[0, n])
        add_window(acc, inner_cur[n], top, left)
        return 0

    lax.fori_loop(0, ready_count, place, 0)

    def shifts(top, left):
        down = {-1: -top, 1: rows - top, 0: None}
        side = {-1: -left, 1: cols - left, 0: None}
        return down, side

    def ranges(at, top, left):
        at_row, at_col = row_id + top, col_id + left
        row_ok = {-1: at_row < 0, 0: (at_row >= 0) & (at_row < rows), 1: at_row >= rows}[at[0]]
        col_ok = {-1: at_col < 0, 0: (at_col >= 0) & (at_col < cols), 1: at_col >= cols}[at[1]]
        return row_ok & col_ok

    def concerns(at, top, left):
        hit = None
        for way in ((at[0], 0), (0, at[1])):
            if way != (0, 0):
                one = crosses(way, top, left, rows, cols)
                hit = one if hit is None else hit & one
        return hit

    def patch(b, slot):
        top, left = corner(slot)
        down, side = shifts(top, left)
        for d, at in enumerate(SHIFTS):
            @pl.when(concerns(at, top, left))
            def _():
                mask = ranges(at, top, left)
                for k in range(2):
                    if at[0] and at[1]:
                        tile = unpacked(halos[at][k], at[1])
                        tile = jnp.concatenate((blank, tile) if at[0] < 0 else (tile, blank), axis=0)
                    elif at[1]:
                        tile = unpacked(halos[at][k, order[2 + d, slot]], at[1])
                    else:
                        tile = halos[at][k, order[2 + d, slot]]
                        tile = jnp.concatenate((blank, tile) if at[0] < 0 else (tile, blank), axis=0)
                    if at[1]:
                        tile = pltpu.roll(tile, side[at[1]], 1)
                    if at[0]:
                        tile = pltpu.roll(tile, down[at[0]], 0)
                    staged[k, b] = jnp.where(mask, tile, staged[k, b])

        res = staged[0, b]
        staged[0, b] = jnp.where(res > 0.0, res, FAR)

    def give(b, slot):
        top, left = corner(slot)
        down, side = shifts(top, left)
        for d, at in enumerate(MAIN):
            @pl.when(concerns(at, top, left))
            def _():
                tile = jnp.where(ranges(at, top, left), solved[b], 0.0)
                if at[1]:
                    tile = pltpu.roll(tile, lax.rem(2 * SIDE - side[at[1]], SIDE), 1)
                    outs[at][order[2 + d, slot]] = (pack_high if at[1] < 0 else pack_low)(tile)
                else:
                    tile = pltpu.roll(tile, lax.rem(2 * SIDE - down[at[0]], SIDE), 0)
                    outs[at][order[2 + d, slot]] = tile[RAD:] if at[0] < 0 else tile[:RAD]

    def solve_group(group, _):
        first = ready_count + group * GROUP
        size = jnp.minimum(live[0] - first, GROUP)

        def ready(b, _):
            n = seat(first + jnp.minimum(b, size - 1))
            staged[0, b] = windows[0, n]
            staged[1, b] = windows[1, n]
            patch(b, order[0, n])
            return 0

        def store(b, cut, current):
            solved[b, cut, :] = current

        def done(b, _):
            slot = order[0, seat(first + b)]
            top, left = corner(slot)
            add_window(acc, solved[b], top, left)
            give(b, slot)
            return 0

        lax.fori_loop(0, GROUP, ready, 0)
        solve(lambda b, cut: (staged[0, b, cut, :], staged[1, b, cut, :]), store)
        lax.fori_loop(0, size, done, 0)
        return 0

    lax.fori_loop(0, (live[0] - ready_count + GROUP - 1) // GROUP, solve_group, 0)
    copy = pltpu.make_async_copy(acc.at[pl.ds(RAD, rows), pl.ds(LANES, cols)], out, out_sem)
    copy.start()
    spans = spans_of(rows, cols)
    for dr, dc in SHIFTS[4:]:
        tile = acc[spans[dr][0], spans[dc][1]]
        outs[(dr, dc)][...] = pack_high(tile) if dc < 0 else pack_low(tile)
    copy.wait()


def reply_kernel(flag, *refs):
    pieces, outs, flag_out = dict(zip(SHIFTS, refs[:8])), dict(zip(SHIFTS, refs[8:16])), refs[16]
    halos = dict(zip(SHIFTS, refs[17:25]))
    flag_landed, send_sems, recv_sems, flag_send, flag_recv = refs[25:]
    found = neighbours()
    peers = peers_along("col")
    for at in SHIFTS:
        halos[at][...] = jnp.zeros_like(halos[at])
    hello(found, SHIFTS, peers)
    wait_for(found, SHIFTS, peers)
    copies = transfers(found, pieces, halos, send_sems, recv_sems)
    start_all(copies)
    shared = share_flag(flag, flag_landed, peers, flag_send, flag_recv)
    for copy in shared:
        copy.start()
    for copy in shared:
        copy.wait()
    flag_out[...] = largest(flag, flag_landed, peers)
    finish_all(copies, landings(found, pieces, halos, send_sems, recv_sems))
    for at in SHIFTS:
        outs[at][...] = halos[at][...]


def settle_kernel(rows, cols, meta, order, *refs):
    halos = dict(zip(SHIFTS, refs[1:9]))
    out, acc, out_sem = refs[9], refs[10], refs[11]
    fetch = pltpu.make_async_copy(out, acc.at[pl.ds(RAD, rows), pl.ds(LANES, cols)], out_sem)
    fetch.start()
    fetch.wait()
    blank = jnp.zeros((RAD, SIDE), jnp.float32)
    for d, at in enumerate(MAIN):
        def add(k, _, d=d, at=at):
            slot = order[6 + d, k]
            top = lax.rem(meta[d, 0, slot], rows) - RAD
            left = lax.rem(meta[d, 1, slot], cols) - RAD
            if at[1]:
                first, second = (to_low if at[1] < 0 else to_high)(halos[at][k])
                tile = jnp.concatenate((first, second), axis=0)
                low = lanes_of(tile.shape) < RAD
                tile = jnp.where(low if at[1] < 0 else jnp.logical_not(low), tile, 0.0)
                add_window(acc, tile, top, 0 if at[1] < 0 else cols - LANES)
            else:
                tile = jnp.concatenate((halos[at][k], blank) if at[0] < 0 else (blank, halos[at][k]), axis=0)
                add_window(acc, tile, 0 if at[0] < 0 else rows - SIDE, left)
            return 0

        lax.fori_loop(0, order[1, 1 + d], add, 0)
    for dr, dc in SHIFTS[4:]:
        first, second = (to_low if dc < 0 else to_high)(halos[(dr, dc)][...])
        low = lanes_of(first.shape) < RAD
        keep = low if dc < 0 else jnp.logical_not(low)
        r = RAD if dr < 0 else rows
        c = LANES if dc < 0 else cols
        for n, part in enumerate((first, second)):
            span = slice(r + RAD // 2 * n, r + RAD // 2 * n + RAD // 2), slice(c, c + LANES)
            acc[span] = acc[span] + jnp.where(keep, part, 0.0)
    store = pltpu.make_async_copy(acc.at[pl.ds(RAD, rows), pl.ds(LANES, cols)], out, out_sem)
    store.start()
    store.wait()


def slow_path(rows, cols, centers, live, raster):
    f32, i32 = jnp.float32, jnp.int32
    smem, vmem, hbm = (pl.BlockSpec(memory_space=m) for m in (pltpu.SMEM, pltpu.VMEM, pltpu.HBM))
    shapes = {
        at: (RAD if at[0] else rows, cols) if at[1] == 0 else ((RAD if at[0] else rows) // 2, LANES) for at in SHIFTS
    }
    pairs = [pltpu.VMEM((2, *shapes[at]), f32) for at in SHIFTS]
    strips = [pltpu.VMEM(shapes[at], f32) for at in SHIFTS]
    stage = [pltpu.VMEM((2, PLANES, SIDE, SIDE), f32), pltpu.VMEM((PLANES, SIDE, SIDE), f32)]
    kinds = (f32, i32, i32)
    frame_shapes = ((rows, LANES), (rows, LANES), (RAD, cols), (RAD, cols))
    halos = pl.pallas_call(
        functools.partial(strips_kernel, rows, cols),
        out_shape=[jax.ShapeDtypeStruct((2, *shapes[at]), f32) for at in SHIFTS],
        in_specs=[hbm] * 3,
        out_specs=[vmem] * 8,
        scratch_shapes=pairs
        + pairs
        + [pltpu.VMEM(shape, kind) for shape in frame_shapes for kind in kinds]
        + [pltpu.SemaphoreType.DMA((4, 3)), pltpu.SemaphoreType.DMA((8,)), pltpu.SemaphoreType.DMA((8,))],
        compiler_params=pltpu.CompilerParams(vmem_limit_bytes=24 << 20, collective_id=3, has_side_effects=True),
        name="strips",
    )(*raster)
    merged, *currents = pl.pallas_call(
        functools.partial(border_kernel, rows, cols),
        out_shape=[jax.ShapeDtypeStruct((rows, cols), f32)]
        + [jax.ShapeDtypeStruct(shapes[at], f32) for at in SHIFTS],
        in_specs=[smem, smem, hbm, hbm, hbm] + [vmem] * 8,
        out_specs=[hbm] + [vmem] * 8,
        scratch_shapes=[pltpu.VMEM((PLANES, TALL + SIDE, WIDE), kind) for kind in kinds]
        + [
            pltpu.SemaphoreType.DMA((3, PLANES)),
            pltpu.VMEM((2, rows + SIDE, cols + WIDE), f32),
            pltpu.VMEM((rows + SIDE, cols + WIDE), f32),
            pltpu.SemaphoreType.DMA,
        ]
        + stage
        + solver_state(PLANES),
        compiler_params=pltpu.CompilerParams(vmem_limit_bytes=42 << 20),
        name="border",
    )(centers, live, *raster, *halos)
    back = pl.pallas_call(
        return_kernel,
        out_shape=[jax.ShapeDtypeStruct(shapes[at], f32) for at in SHIFTS],
        in_specs=[vmem] * 8,
        out_specs=[vmem] * 8,
        scratch_shapes=strips + [pltpu.SemaphoreType.DMA((8,)), pltpu.SemaphoreType.DMA((8,))],
        compiler_params=pltpu.CompilerParams(vmem_limit_bytes=8 << 20, collective_id=4, has_side_effects=True),
        name="give_back",
    )(*currents)
    return pl.pallas_call(
        functools.partial(fold_kernel, rows, cols),
        out_shape=jax.ShapeDtypeStruct((rows, cols), f32),
        in_specs=[hbm] + [vmem] * 8,
        out_specs=hbm,
        scratch_shapes=[
            pltpu.VMEM((RAD, cols), f32),
            pltpu.VMEM((RAD, cols), f32),
            pltpu.VMEM((rows - SIDE, LANES), f32),
            pltpu.VMEM((rows - SIDE, LANES), f32),
            pltpu.SemaphoreType.DMA((2, 4)),
        ],
        input_output_aliases={0: 0},
        compiler_params=pltpu.CompilerParams(vmem_limit_bytes=16 << 20),
        name="fold",
    )(merged, *back)


def local(resistance, source_mask, target_mask, centers, live):
    rows, cols = resistance.shape
    raster = (resistance, source_mask, target_mask)
    centers = centers.T
    slots = centers.shape[1]
    f32, i32 = jnp.float32, jnp.int32
    smem, vmem, hbm = (pl.BlockSpec(memory_space=m) for m in (pltpu.SMEM, pltpu.VMEM, pltpu.HBM))
    dma = pltpu.SemaphoreType.DMA
    kinds = (f32, i32, i32)
    piece = {at: (RAD // 2, LANES) if at[0] and at[1] else (PIECES, RAD, LANES) for at in SHIFTS}
    twice = [(2, *piece[at]) for at in SHIFTS]
    flag_shape = jax.ShapeDtypeStruct((8, LANES), i32)
    row_peers, col_peers = lax.axis_size("row") - 1, lax.axis_size("col") - 1

    meta = pl.pallas_call(
        meta_kernel,
        out_shape=jax.ShapeDtypeStruct((len(MAIN), 8, LANES), i32),
        in_specs=[smem, smem],
        out_specs=vmem,
        scratch_shapes=[pltpu.VMEM((8, LANES), i32), pltpu.VMEM((len(MAIN), 8, LANES), i32), dma((8,)), dma((8,))],
        compiler_params=pltpu.CompilerParams(vmem_limit_bytes=1 << 20, collective_id=0, has_side_effects=True),
        name="meta",
    )(centers, live)

    windows, order, *rest = pl.pallas_call(
        functools.partial(pack_kernel, rows, cols),
        out_shape=[jax.ShapeDtypeStruct((2, slots, SIDE, SIDE), f32), jax.ShapeDtypeStruct((10, slots), i32)]
        + [jax.ShapeDtypeStruct(shape, f32) for shape in twice]
        + [flag_shape],
        in_specs=[smem, smem, smem, hbm, hbm, hbm],
        out_specs=[vmem, smem] + [vmem] * 9,
        scratch_shapes=[pltpu.VMEM((slots, TALL, WIDE), kind) for kind in kinds]
        + [pltpu.VMEM((len(MAIN), PIECES, TALL, WIDE), kind) for kind in kinds]
        + [pltpu.VMEM((4, RAD, LANES), kind) for kind in kinds]
        + [dma((3, slots)), dma((3, len(MAIN), PIECES)), dma((3, 4))],
        compiler_params=pltpu.CompilerParams(vmem_limit_bytes=40 << 20),
        name="pack",
    )(centers, live, meta, *raster)
    pieces, flag = rest[:8], rest[8]

    inner_cur, *rest = pl.pallas_call(
        trade_kernel,
        out_shape=[jax.ShapeDtypeStruct((GROUP, SIDE, SIDE), f32)]
        + [jax.ShapeDtypeStruct(shape, f32) for shape in twice]
        + [flag_shape],
        in_specs=[vmem] * 10,
        out_specs=[vmem] * 10,
        scratch_shapes=[pltpu.VMEM(shape, f32) for shape in twice]
        + [pltpu.VMEM((row_peers, 8, LANES), i32), dma((8,)), dma((8,)), dma((row_peers,)), dma((row_peers,))]
        + solver_state(GROUP),
        compiler_params=pltpu.CompilerParams(vmem_limit_bytes=32 << 20, collective_id=1, has_side_effects=True),
        name="trade",
    )(windows, flag, *pieces)
    halos, flag = rest[:8], rest[8]

    merged, *pieces = pl.pallas_call(
        functools.partial(rest_kernel, rows, cols),
        out_shape=[jax.ShapeDtypeStruct((rows, cols), f32)]
        + [jax.ShapeDtypeStruct(piece[at], f32) for at in SHIFTS],
        in_specs=[smem, smem, smem] + [vmem] * 10,
        out_specs=[hbm] + [vmem] * 8,
        scratch_shapes=[pltpu.VMEM((rows + SIDE, cols + WIDE), f32), dma]
        + [pltpu.VMEM((2, GROUP, SIDE, SIDE), f32), pltpu.VMEM((GROUP, SIDE, SIDE), f32)]
        + solver_state(GROUP),
        compiler_params=pltpu.CompilerParams(vmem_limit_bytes=40 << 20),
        name="rest",
    )(centers, live, order, windows, inner_cur, *halos)

    *halos, flag = pl.pallas_call(
        reply_kernel,
        out_shape=[jax.ShapeDtypeStruct(piece[at], f32) for at in SHIFTS] + [flag_shape],
        in_specs=[vmem] * 9,
        out_specs=[vmem] * 9,
        scratch_shapes=[pltpu.VMEM(piece[at], f32) for at in SHIFTS]
        + [pltpu.VMEM((col_peers, 8, LANES), i32), dma((8,)), dma((8,)), dma((col_peers,)), dma((col_peers,))],
        compiler_params=pltpu.CompilerParams(vmem_limit_bytes=8 << 20, collective_id=2, has_side_effects=True),
        name="reply",
    )(flag, *pieces)

    def quick():
        return pl.pallas_call(
            functools.partial(settle_kernel, rows, cols),
            out_shape=jax.ShapeDtypeStruct((rows, cols), f32),
            in_specs=[smem, smem, hbm] + [vmem] * 8,
            out_specs=hbm,
            scratch_shapes=[pltpu.VMEM((rows + SIDE, cols + WIDE), f32), dma],
            input_output_aliases={2: 0},
            compiler_params=pltpu.CompilerParams(vmem_limit_bytes=16 << 20),
            name="settle",
        )(meta, order, merged, *halos)

    return lax.cond(flag[0, 0] > 0, lambda: slow_path(rows, cols, centers, live, raster), quick)


def solution(mesh):
    return jax.shard_map(
        local,
        mesh=mesh,
        in_specs=(
            P("row", "col"),
            P("row", "col"),
            P("row", "col"),
            P(("row", "col"), None),
            P(("row", "col")),
        ),
        out_specs=P("row", "col"),
        check_vma=False,
    )
```

```python
import functools

import jax
import jax.numpy as jnp
from jax import lax
from jax.experimental import pallas as pl
from jax.experimental.pallas import tpu as pltpu
from jax.sharding import PartitionSpec as P

RAD = 64
SIDE = 2 * RAD
ITERS = 24
LEAKAGE = 0.02
FAR = 1e37
GROUP = 8
LANES = 128
TALL = SIDE + 8
WIDE = 2 * LANES
SHIFTS = ((0, -1), (0, 1), (-1, 0), (1, 0), (-1, -1), (-1, 1), (1, -1), (1, 1))


def roll(value, shift, axis):
    return pltpu.roll(value, shift % value.shape[axis], axis)


def lane_ids(shape):
    return lax.broadcasted_iota(jnp.int32, shape, 1)


def to_low(packed):
    return packed, roll(packed, RAD, 1)


def to_high(packed):
    return roll(packed, RAD, 1), packed


def pack_low(tile):
    half = tile.shape[0] // 2
    first, second = tile[:half], tile[half:]
    return jnp.where(lane_ids(first.shape) < RAD, first, roll(second, RAD, 1))


def pack_high(tile):
    half = tile.shape[0] // 2
    first, second = tile[:half], tile[half:]
    return jnp.where(lane_ids(first.shape) < RAD, roll(first, RAD, 1), second)


def neighbours():
    row, col = lax.axis_index("row"), lax.axis_index("col")
    rows, cols = lax.axis_size("row"), lax.axis_size("col")
    found = {}
    for (dr, dc) in SHIFTS:
        r, c = row + dr, col + dc
        found[(dr, dc)] = ((r >= 0) & (r < rows) & (c >= 0) & (c < cols), (r, c))
    return found


def greet(found):
    barrier = pltpu.get_barrier_semaphore()
    for at in SHIFTS:
        exists, device = found[at]

        @pl.when(exists)
        def _():
            pl.semaphore_signal(barrier, inc=1, device_id=device, device_id_type=pl.DeviceIdType.MESH)


def all_greeted(found):
    count = sum(found[at][0].astype(jnp.int32) for at in SHIFTS)
    pl.semaphore_wait(pltpu.get_barrier_semaphore(), count)


def transfers(found, pieces, halos, send_sems, recv_sems, ats=SHIFTS):
    made = []
    for at in ats:
        k = SHIFTS.index(at)
        exists, device = found[at]
        back = (-at[0], -at[1])
        made.append((exists, pltpu.make_async_remote_copy(
            src_ref=pieces[at],
            dst_ref=halos[back],
            send_sem=send_sems.at[k],
            recv_sem=recv_sems.at[SHIFTS.index(back)],
            device_id=device,
            device_id_type=pl.DeviceIdType.MESH,
        )))
    return made


def landings(found, pieces, halos, send_sems, recv_sems, ats=SHIFTS):
    made = []
    for at in ats:
        k = SHIFTS.index(at)
        exists, device = found[at]
        made.append((exists, pltpu.make_async_remote_copy(
            src_ref=pieces[at],
            dst_ref=halos[at],
            send_sem=send_sems.at[k],
            recv_sem=recv_sems.at[k],
            device_id=device,
            device_id_type=pl.DeviceIdType.MESH,
        )))
    return made


def start_all(copies):
    for exists, copy in copies:
        pl.when(exists)(copy.start)


def finish_all(copies, arrivals):
    for exists, copy in copies:
        pl.when(exists)(copy.wait_send)
    for exists, copy in arrivals:
        pl.when(exists)(copy.wait_recv)


def corner_of(centers, slot, rows, cols):
    return lax.rem(centers[0, slot], rows) - RAD, lax.rem(centers[1, slot], cols) - RAD


def is_inner(top, left, rows, cols):
    return (top >= 0) & (top <= rows - SIDE) & (left >= 0) & (left <= cols - SIDE)


def clamped(top, left, rows, cols):
    row = jnp.clip((top + RAD) // 8 * 8 - RAD, 0, rows - TALL)
    col = jnp.clip((left + LANES) // LANES * LANES - LANES, 0, cols - WIDE)
    return pl.multiple_of(row, 8), pl.multiple_of(col, LANES)


def total(values):
    return jnp.sum(jnp.sum(values, axis=0, keepdims=True), axis=1, keepdims=True)


def cut_rows(value, skip):
    return pltpu.roll(value, lax.rem(TALL - skip, TALL), 0)[:SIDE]


def add_window(acc, current, top, left):
    col = pl.multiple_of((left + LANES) // LANES * LANES, LANES)
    shift = left + LANES - col
    wide = jnp.concatenate([current, jnp.zeros_like(current)], axis=1)
    wide = pltpu.roll(wide, shift, 1)
    wide = jnp.concatenate([wide, jnp.zeros((8, WIDE), jnp.float32)], axis=0)
    wide = pltpu.roll(wide, lax.rem(top + RAD, 8), 0)
    rows = pl.ds(pl.multiple_of((top + RAD) // 8 * 8, 8), TALL)
    acc[rows, pl.ds(col, WIDE)] = acc[rows, pl.ds(col, WIDE)] + wide


PLANES = 4
CHUNK = 64
SEGMENTS = SIDE // PLANES
EIGHTS = tuple(slice(8 * k, 8 * k + 8) for k in range(SIDE // 8))


def lanes_of(shape):
    return lax.broadcasted_iota(jnp.int32, shape, 1)


def interleave(shape, transposed):
    row, col = (lax.broadcasted_iota(jnp.int32, shape, axis) for axis in (0, 1))
    if transposed:
        row, col = col, row
    window, place = row // SIDE, row % SIDE
    return (col == (place % PLANES) * SIDE + window * SEGMENTS + place // PLANES).astype(jnp.bfloat16)


def halves(value):
    high = value.astype(jnp.bfloat16)
    return high, (value - high.astype(jnp.float32)).astype(jnp.bfloat16)


def mixed(parts, table):
    found = jnp.dot(jnp.concatenate(parts, axis=0), table[...], preferred_element_type=jnp.float32)
    size = parts[0].shape[0]
    return [found[size * n:size * n + size] for n in range(len(parts))]


def quad_state():
    f32 = jnp.float32
    planes = pltpu.VMEM((PLANES, SIDE, SIDE), f32)
    padded = pltpu.VMEM((PLANES, SIDE + 16, SIDE), f32)
    tile = pltpu.VMEM((SIDE, SIDE), f32)
    table = pltpu.VMEM((ITERS, 8, SIDE), f32)
    return (
        [padded, padded, pltpu.VMEM((ITERS, PLANES, SIDE, SIDE), f32), planes]
        + [padded, planes, tile]
        + [tile, tile]
        + [padded, planes, planes, padded, padded, planes]
        + [table, table]
    )


def solver_state(group, table=True):
    wide = PLANES * SIDE
    states = quad_state() * (group // PLANES)
    return states + [pltpu.VMEM((2, wide, wide), jnp.bfloat16)] if table else states


def quad_parts(state):
    even, odd, hist, t_s, vert, hori, hori_in, edge_r, edge_l, isd_s, inj_s, gnd_s, v_s, res_s, h_s, tail_s, link_s = state
    f32 = jnp.float32
    mid = tuple(slice(8 + 8 * k, 16 + 8 * k) for k in range(SIDE // 8))
    low = tuple(slice(9 + 8 * k, 17 + 8 * k) for k in range(SIDE // 8))
    upp = tuple(slice(7 + 8 * k, 15 + 8 * k) for k in range(SIDE // 8))
    blocks = range(SIDE // 8)
    lane = lanes_of((8, SIDE))
    row8 = lax.broadcasted_iota(jnp.int32, (8, SIDE), 0)

    def clear():
        zero = jnp.zeros((8, SIDE), f32)
        for pad in (even, odd, vert, isd_s, v_s, res_s):
            for p in range(PLANES):
                pad[p, 0:8, :] = zero
                pad[p, 8 + SIDE:16 + SIDE, :] = zero

    def refresh_edges(cur):
        for k in blocks:
            edge_r[EIGHTS[k], :] = roll(cur[0, mid[k], :], -1, 1)
            edge_l[EIGHTS[k], :] = roll(cur[PLANES - 1, mid[k], :], 1, 1)

    def operate(cur):
        gammas, deltas = [None] * PLANES, [None] * PLANES
        for k in blocks:
            here = [cur[p, mid[k], :] for p in range(PLANES)]
            out = [hori[p, EIGHTS[k], :] for p in range(PLANES)]
            for p in (1, 2, 0, 3):
                right = here[p + 1] if p < PLANES - 1 else edge_r[EIGHTS[k], :]
                left = here[p - 1] if p else edge_l[EIGHTS[k], :]
                back = out[p - 1] if p else hori_in[EIGHTS[k], :]
                beside = vert[p, mid[k], :] * cur[p, low[k], :] + vert[p, upp[k], :] * cur[p, upp[k], :]
                beside = beside + (out[p] * right + back * left)
                t_s[p, EIGHTS[k], :] = beside
                one, two = here[p] * here[p], here[p] * beside
                gammas[p] = one if k == 0 else gammas[p] + one
                deltas[p] = two if k == 0 else deltas[p] + two
        return (gammas[0] + gammas[1]) + (gammas[2] + gammas[3]), (deltas[0] + deltas[1]) + (deltas[2] + deltas[3])

    def down_sum(part):
        for shift in (4, 2, 1):
            part = part + roll(part, shift, 0)
        return part

    def total_of(sums):
        mine = lane // SEGMENTS == row8 % PLANES
        first = row8 < PLANES
        both = jnp.where(first, down_sum(sums[0]), down_sum(sums[1]))
        both = jnp.where(mine, jnp.sum(jnp.where(mine, both, 0.0), axis=1, keepdims=True), 0.0)
        return down_sum(jnp.where(first, both, 0.0)), down_sum(jnp.where(first, 0.0, both))

    def prepare(load, table):
        for r in range(0, SIDE, CHUNK):
            cut = slice(r, r + CHUNK)
            loaded = [load(w, cut) for w in range(PLANES)]
            res = jnp.concatenate([pair[0] for pair in loaded], axis=1)
            mark = jnp.concatenate([pair[1] for pair in loaded], axis=1)
            high, low_part, mark = mixed([*halves(res), mark.astype(jnp.bfloat16)], table)
            res = high + low_part
            signed = mark / res
            for p in range(PLANES):
                span = slice(SIDE * p, SIDE * p + SIDE)
                res_s[p, 8 + r:8 + r + CHUNK, :] = res[:, span]
                inject = jnp.maximum(signed[:, span], 0.0)
                if p == 0 and r <= RAD < r + CHUNK:
                    at = lax.broadcasted_iota(jnp.int32, (CHUNK, SIDE), 0) == RAD - r
                    spot = lanes_of((CHUNK, SIDE)) % SEGMENTS == RAD // PLANES
                    inject = inject + (at & spot).astype(f32)
                inj_s[p, cut, :] = inject
                gnd_s[p, cut, :] = jnp.maximum(-signed[:, span], 0.0)
        ends = lane % SEGMENTS == SEGMENTS - 1
        bottom = row8 == 7
        for k in blocks:
            for p in range(PLANES):
                here = res_s[p, mid[k], :]
                under = res_s[p, low[k], :]
                if k == len(EIGHTS) - 1:
                    vertical = jnp.where(bottom, 0.0, 2.0 / (here + jnp.where(bottom, FAR, under)))
                else:
                    vertical = 2.0 / (here + under)
                v_s[p, mid[k], :] = vertical
                if p < PLANES - 1:
                    h_s[p, EIGHTS[k], :] = 2.0 / (here + res_s[p + 1, mid[k], :])
                else:
                    horizontal = jnp.where(ends, 0.0, 2.0 / (here + roll(res_s[0, mid[k], :], -1, 1)))
                    h_s[p, EIGHTS[k], :] = horizontal
                    edge_l[EIGHTS[k], :] = roll(horizontal, 1, 1)
        for k in blocks:
            for p in range(PLANES):
                before = h_s[p - 1, EIGHTS[k], :] if p else edge_l[EIGHTS[k], :]
                diagonal = v_s[p, mid[k], :] + v_s[p, upp[k], :] + (h_s[p, EIGHTS[k], :] + before)
                isd_s[p, mid[k], :] = 1.0 / jnp.sqrt(diagonal + gnd_s[p, EIGHTS[k], :] + LEAKAGE)
        for k in blocks:
            for p in range(PLANES):
                isd = isd_s[p, mid[k], :]
                vert[p, mid[k], :] = v_s[p, mid[k], :] * isd * isd_s[p, low[k], :]
                if p < PLANES - 1:
                    hori[p, EIGHTS[k], :] = h_s[p, EIGHTS[k], :] * isd * isd_s[p + 1, mid[k], :]
                else:
                    scaled = h_s[p, EIGHTS[k], :] * isd * roll(isd_s[0, mid[k], :], -1, 1)
                    hori[p, EIGHTS[k], :] = scaled
                    hori_in[EIGHTS[k], :] = roll(scaled, 1, 1)
                first = inj_s[p, EIGHTS[k], :] * isd
                even[p, mid[k], :] = first
                hist[0, p, EIGHTS[k], :] = first
        refresh_edges(even)
        return operate(even)

    def settle(j, sums, gamma_inv_before, pivot_inv, weight):
        gamma, delta = sums
        gamma_inv = 1.0 / gamma
        mean = delta * gamma_inv
        ratio = gamma * gamma_inv_before
        link = ratio * pivot_inv
        pivot_inv = 1.0 / (1.0 - mean - link)
        weight = weight * pivot_inv
        tail_s[j] = weight
        link_s[j] = link
        return mean, ratio, gamma_inv, pivot_inv, weight

    def update(j, way, mean, ratio):
        cur, new = (odd, even) if way else (even, odd)
        for p in (0, 3, 1, 2):
            for k in blocks:
                fresh = t_s[p, EIGHTS[k], :] - mean * cur[p, mid[k], :]
                if ratio is not None:
                    fresh = fresh - ratio * new[p, mid[k], :]
                new[p, mid[k], :] = fresh
                hist[j + 1, p, EIGHTS[k], :] = fresh
                if p == 0:
                    edge_r[EIGHTS[k], :] = roll(fresh, -1, 1)
                if p == PLANES - 1:
                    edge_l[EIGHTS[k], :] = roll(fresh, 1, 1)
        return operate(new)

    def coefficients():
        factor = tail_s[ITERS - 1]
        for j in reversed(range(1, ITERS)):
            ahead = tail_s[j - 1] + link_s[j] * factor
            tail_s[j] = factor
            factor = ahead
        tail_s[0] = factor

    def voltages():
        def one(p, _):
            for half in range(2):
                found = [None] * 8
                for j in range(ITERS):
                    factor = tail_s[j]
                    for i in range(8):
                        term = factor * hist[j, p, EIGHTS[8 * half + i], :]
                        found[i] = term if found[i] is None else found[i] + term
                for i in range(8):
                    even[p, mid[8 * half + i], :] = found[i] * isd_s[p, mid[8 * half + i], :]
            return 0

        lax.fori_loop(0, PLANES, one, 0)

    def finish(put, table):
        cur = even
        for k in blocks:
            edge_r[EIGHTS[k], :] = roll(cur[0, mid[k], :], -1, 1)
        for k in blocks:
            for p in range(PLANES):
                volts = cur[p, mid[k], :]
                res_s[p, mid[k], :] = v_s[p, mid[k], :] * jnp.abs(volts - cur[p, low[k], :])
                right = cur[p + 1, mid[k], :] if p < PLANES - 1 else edge_r[EIGHTS[k], :]
                flow = h_s[p, EIGHTS[k], :] * jnp.abs(volts - right)
                t_s[p, EIGHTS[k], :] = flow
                if p == PLANES - 1:
                    edge_l[EIGHTS[k], :] = roll(flow, 1, 1)

        for r in range(0, SIDE, CHUNK):
            cut = slice(r, r + CHUNK)
            pieces = []
            for p in range(PLANES):
                flow = res_s[p, 8 + r:8 + r + CHUNK, :] + res_s[p, 7 + r:7 + r + CHUNK, :] + t_s[p, cut, :]
                flow = flow + (t_s[p - 1, cut, :] if p else edge_l[cut, :])
                pieces.append(0.5 * (flow + inj_s[p, cut, :] + gnd_s[p, cut, :] * jnp.abs(cur[p, 8 + r:8 + r + CHUNK, :])))
            high, low_part = mixed(halves(jnp.concatenate(pieces, axis=1)), table)
            for w in range(PLANES):
                span = slice(SIDE * w, SIDE * w + SIDE)
                put(w, cut, high[:, span] + low_part[:, span])

    return clear, prepare, total_of, operate, settle, update, coefficients, voltages, finish


def solver_parts(state, group):
    table = state[-1]
    count = group // PLANES
    size = len(quad_state())
    quads = [quad_parts(state[size * q:size * q + size]) for q in range(count)]

    def clear():
        for quad in quads:
            quad[0]()

    def tables():
        for way in range(2):
            table[way] = interleave(table.shape[1:], way == 1)

    def solve(load, store):
        one = jnp.ones((8, SIDE), jnp.float32)
        carry = []
        for q, (_, prepare, total_of, *_) in enumerate(quads):
            sums = prepare(lambda w, cut, q=q: load(PLANES * q + w, cut), table.at[0])
            carry.append((sums if q else total_of(sums), 0.0 * one, 0.0 * one, one))

        def step(j, way, carry, first=False):
            after = []
            for q, (_, _, total_of, operate, settle, update, *_) in enumerate(quads):
                sums, *rest = carry[q]
                if q:
                    sums = total_of(sums)
                mean, ratio, *rest = settle(j, sums, *rest)
                sums = update(j, way, mean, None if first else ratio)
                after.append((sums if q else total_of(sums), *rest))
            return after

        def steps(i, carry):
            return tuple(step(2 * i + 2, 0, step(2 * i + 1, 1, carry)))

        carry = tuple(step(0, 0, carry, True))
        carry = lax.fori_loop(0, (ITERS - 2) // 2, steps, carry)
        for q, (_, _, total_of, _, settle, _, coefficients, *_) in enumerate(quads):
            settle(ITERS - 1, total_of(carry[q][0]) if q else carry[q][0], *carry[q][1:])
            coefficients()
        for *_, voltages, _ in quads:
            voltages()
        for q, (*_, finish) in enumerate(quads):
            finish(lambda w, cut, tile, q=q: store(PLANES * q + w, cut, tile), table.at[1])

    return clear, tables, solve


def spans_of(rows, cols):
    return {
        -1: (slice(0, RAD), slice(0, LANES)),
        0: (slice(RAD, RAD + rows), slice(LANES, LANES + cols)),
        1: (slice(RAD + rows, SIDE + rows), slice(LANES + cols, WIDE + cols)),
    }


def mark_of(source, target):
    source, target = source.astype(jnp.float32), target.astype(jnp.float32)
    return source - target * (1.0 - source)


def turn_own(res, source, target, skip, turn):
    source, target = source.astype(jnp.float32), target.astype(jnp.float32)
    mark = source - target * (1.0 - source)
    turn = lax.rem(WIDE + turn, WIDE)
    res = cut_rows(pltpu.roll(res, turn, 1)[:, :SIDE], skip)
    mark = cut_rows(pltpu.roll(mark, turn, 1)[:, :SIDE], skip)
    return res, mark


def strips_kernel(rows, cols, *refs):
    raw = refs[:3]
    outs = dict(zip(SHIFTS, refs[3:11]))
    pieces, halos = dict(zip(SHIFTS, refs[11:19])), dict(zip(SHIFTS, refs[19:27]))
    frames = [refs[27 + 3 * k:30 + 3 * k] for k in range(4)]
    sems, send_sems, recv_sems = refs[39:42]
    found = neighbours()

    everything = pl.ds(0, rows)
    places = (
        (everything, pl.ds(0, LANES)),
        (everything, pl.ds(cols - LANES, LANES)),
        (pl.ds(0, RAD), pl.ds(0, cols)),
        (pl.ds(rows - RAD, RAD), pl.ds(0, cols)),
    )
    frame_copies = [
        [pltpu.make_async_copy(raw[k].at[places[f]], frames[f][k], sems.at[f, k]) for k in range(3)]
        for f in range(4)
    ]
    for copy in sum(frame_copies, []):
        copy.start()
    for at in SHIFTS:
        halos[at][...] = jnp.zeros_like(halos[at])
    greet(found)

    def strengths(frame, cut=slice(None)):
        res, source, target = (ref[cut] for ref in frame)
        source, target = source.astype(jnp.float32), target.astype(jnp.float32)
        return res, source - target * (1.0 - source)

    for f, at in enumerate(((0, -1), (0, 1), (-1, 0), (1, 0))):
        for copy in frame_copies[f]:
            copy.wait()
        for k, value in enumerate(strengths(frames[f])):
            if at[1] == 0:
                pieces[at][k] = value
            else:
                squeeze = pack_low if at[1] < 0 else pack_high
                pieces[at][k] = squeeze(value)
                pieces[(-1, at[1])][k] = squeeze(value[:RAD])
                pieces[(1, at[1])][k] = squeeze(value[rows - RAD:])
    all_greeted(found)
    copies = transfers(found, pieces, halos, send_sems, recv_sems)
    start_all(copies)

    finish_all(copies, landings(found, pieces, halos, send_sems, recv_sems))
    for at in SHIFTS:
        outs[at][...] = halos[at][...]


def return_kernel(*refs):
    pieces, outs, halos = (dict(zip(SHIFTS, refs[8 * k:8 * k + 8])) for k in range(3))
    send_sems, recv_sems = refs[24:]
    found = neighbours()
    for at in SHIFTS:
        halos[at][...] = jnp.zeros_like(halos[at])
    greet(found)
    all_greeted(found)
    copies = transfers(found, pieces, halos, send_sems, recv_sems)
    start_all(copies)
    finish_all(copies, landings(found, pieces, halos, send_sems, recv_sems))
    for at in SHIFTS:
        outs[at][...] = halos[at][...]


def border_kernel(rows, cols, centers, live, *refs):
    raw, halos = refs[:3], dict(zip(SHIFTS, refs[3:11]))
    out, outs = refs[11], dict(zip(SHIFTS, refs[12:20]))
    bufs, sems, ext, acc, out_sem, staged, solved = refs[20:23], *refs[23:29]
    clear, tables, solve = solver_parts(refs[29:], PLANES)

    def copies(slot, at):
        top, left = corner_of(centers, slot, rows, cols)
        row, col = clamped(top, left, rows, cols)
        return [
            pltpu.make_async_copy(
                src.at[pl.ds(row, TALL), pl.ds(col, WIDE)],
                dst.at[at, pl.ds(RAD, TALL), :],
                sems.at[k, at],
            )
            for k, (src, dst) in enumerate(zip(raw, bufs))
        ]

    count = live[0]
    acc[...] = jnp.zeros_like(acc)
    clear()
    tables()
    spans = spans_of(rows, cols)
    for which in range(2):
        for dr in (-1, 1):
            ext[which, spans[dr][0], spans[0][1]] = halos[(dr, 0)][which]
        for dr in (-1, 0, 1):
            start, stop = spans[dr][0].start, spans[dr][0].stop
            middle = (start + stop) // 2
            for dc in (-1, 1):
                split = to_high if dc < 0 else to_low
                first, second = split(halos[(dr, dc)][which])
                ext[which, start:middle, spans[dc][1]] = first
                ext[which, middle:stop, spans[dc][1]] = second

    row_id = lax.broadcasted_iota(jnp.int32, (SIDE, SIDE), 0)
    col_id = lax.broadcasted_iota(jnp.int32, (SIDE, SIDE), 1)

    def fetch(slot, b):
        top, left = corner_of(centers, slot, rows, cols)
        row, col = clamped(top, left, rows, cols)
        take = pl.ds(pl.multiple_of((RAD + top - row) // 8 * 8, 8), TALL)
        res, source, target = (buf[b, take, :] for buf in bufs)
        res, mark = turn_own(res, source, target, lax.rem(RAD + top - row, 8), col - left)
        at_row, at_col = row_id + top, col_id + left
        own = (at_row >= 0) & (at_row < rows) & (at_col >= 0) & (at_col < cols)
        base = pl.multiple_of((left + LANES) // LANES * LANES, LANES)
        back = lax.rem(WIDE + base - left - LANES, WIDE)
        span = pl.ds(pl.multiple_of((top + RAD) // 8 * 8, 8), TALL)
        outer = [
            cut_rows(pltpu.roll(ext[k, span, pl.ds(base, WIDE)], back, 1)[:, :SIDE], lax.rem(top + RAD, 8))
            for k in range(2)
        ]
        res = jnp.where(own, res, outer[0])
        return jnp.where(res > 0.0, res, FAR), jnp.where(own, mark, outer[1])

    def solve_group(group, _):
        size = jnp.minimum(count - group * PLANES, PLANES)

        def begin(b, _):
            for copy in copies((group * PLANES + b), b):
                copy.start()
            return 0

        def ready(b, _):
            b_own = jnp.minimum(b, size - 1)
            slot = (group * PLANES + b_own)

            @pl.when(b < size)
            def _():
                for copy in copies(slot, b):
                    copy.wait()

            staged[0, b], staged[1, b] = fetch(slot, b_own)
            return 0

        def store(b, cut, current):
            solved[b, cut, :] = current

        def done(b, _):
            top, left = corner_of(centers, (group * PLANES + b), rows, cols)
            add_window(acc, solved[b], top, left)
            return 0

        lax.fori_loop(0, size, begin, 0)
        lax.fori_loop(0, PLANES, ready, 0)
        solve(lambda b, cut: (staged[0, b, cut, :], staged[1, b, cut, :]), store)
        lax.fori_loop(0, size, done, 0)
        return 0

    lax.fori_loop(0, (count + PLANES - 1) // PLANES, solve_group, 0)

    copy = pltpu.make_async_copy(acc.at[pl.ds(RAD, rows), pl.ds(LANES, cols)], out, out_sem)
    copy.start()
    for dr in (-1, 1):
        outs[(dr, 0)][...] = acc[spans[dr][0], spans[0][1]]
    for dr in (-1, 0, 1):
        for dc in (-1, 1):
            tile = acc[spans[dr][0], spans[dc][1]]
            outs[(dr, dc)][...] = pack_high(tile) if dc < 0 else pack_low(tile)
    copy.wait()


def fold_kernel(rows, cols, *refs):
    halos = dict(zip(SHIFTS, refs[1:9]))
    out, upper, lower, left, right, sems = refs[9:]
    last = cols - LANES
    inner_rows = rows - SIDE
    places = (
        (upper, pl.ds(0, RAD), pl.ds(0, cols)),
        (lower, pl.ds(rows - RAD, RAD), pl.ds(0, cols)),
        (left, pl.ds(RAD, inner_rows), pl.ds(0, LANES)),
        (right, pl.ds(RAD, inner_rows), pl.ds(last, LANES)),
    )
    fetch = [pltpu.make_async_copy(out.at[r, c], buf, sems.at[0, k]) for k, (buf, r, c) in enumerate(places)]
    store = [pltpu.make_async_copy(buf, out.at[r, c], sems.at[1, k]) for k, (buf, r, c) in enumerate(places)]
    for copy in fetch:
        copy.start()

    def spread(dr, dc):
        first, second = (to_low if dc < 0 else to_high)(halos[(dr, dc)][...])
        low = lane_ids(first.shape) < RAD
        keep = low if dc < 0 else jnp.logical_not(low)
        return jnp.where(keep, first, 0.0), jnp.where(keep, second, 0.0)

    for copy in fetch:
        copy.wait()
    half = rows // 2
    for dc, buf, at in ((-1, left, 0), (1, right, last)):
        first, second = spread(0, dc)
        buf[0:half - RAD] = buf[0:half - RAD] + first[RAD:]
        buf[half - RAD:inner_rows] = buf[half - RAD:inner_rows] + second[:half - RAD]
        upper[:, at:at + LANES] = upper[:, at:at + LANES] + first[:RAD]
        lower[:, at:at + LANES] = lower[:, at:at + LANES] + second[half - RAD:]
        for dr, strip in ((-1, upper), (1, lower)):
            one, two = spread(dr, dc)
            strip[:RAD // 2, at:at + LANES] = strip[:RAD // 2, at:at + LANES] + one
            strip[RAD // 2:, at:at + LANES] = strip[RAD // 2:, at:at + LANES] + two
    upper[...] = upper[...] + halos[(-1, 0)][...]
    lower[...] = lower[...] + halos[(1, 0)][...]
    for copy in store:
        copy.start()
    for copy in store:
        copy.wait()


MAIN = SHIFTS[:4]
PIECES = 4


def wait_for(found, ats, peers):
    count = sum(found[at][0].astype(jnp.int32) for at in ats) + len(peers)
    pl.semaphore_wait(pltpu.get_barrier_semaphore(), count)


def hello(found, ats, peers):
    barrier = pltpu.get_barrier_semaphore()
    for at in ats:
        exists, device = found[at]

        @pl.when(exists)
        def _():
            pl.semaphore_signal(barrier, inc=1, device_id=device, device_id_type=pl.DeviceIdType.MESH)

    for device in peers:
        pl.semaphore_signal(barrier, inc=1, device_id=device, device_id_type=pl.DeviceIdType.MESH)


def peers_along(axis):
    row, col = lax.axis_index("row"), lax.axis_index("col")
    size = lax.axis_size(axis)
    if axis == "row":
        return [(lax.rem(row + k, size), col) for k in range(1, size)]
    return [(row, lax.rem(col + k, size)) for k in range(1, size)]


def share_flag(flag, landed, peers, send_sems, recv_sems):
    return [
        pltpu.make_async_remote_copy(
            src_ref=flag, dst_ref=landed.at[k], send_sem=send_sems.at[k], recv_sem=recv_sems.at[k],
            device_id=device, device_id_type=pl.DeviceIdType.MESH,
        )
        for k, device in enumerate(peers)
    ]


def largest(flag, landed, peers):
    found = flag[...]
    for k in range(len(peers)):
        found = jnp.maximum(found, landed[k])
    return found


def meta_kernel(centers, live, out, mine, halos, send_sems, recv_sems):
    found = neighbours()
    halos[...] = jnp.zeros_like(halos)
    hello(found, MAIN, [])
    slots = centers.shape[1]
    row8 = lax.broadcasted_iota(jnp.int32, (8, LANES), 0)
    lane8 = lanes_of((8, LANES))
    block = jnp.broadcast_to(live[0], (8, LANES)).astype(jnp.int32)
    for s in range(slots):
        for axis in range(2):
            block = jnp.where((row8 == axis) & (lane8 == s), centers[axis, s], block)
    mine[...] = block
    wait_for(found, MAIN, [])
    args = (found, {at: mine for at in MAIN}, {at: halos.at[k] for k, at in enumerate(MAIN)}, send_sems, recv_sems)
    copies = transfers(*args, ats=MAIN)
    start_all(copies)
    finish_all(copies, landings(*args, ats=MAIN))
    out[...] = halos[...]


def crosses(at, top, left, rows, cols):
    tests = {(0, -1): left < 0, (0, 1): left + SIDE > cols, (-1, 0): top < 0, (1, 0): top + SIDE > rows}
    return tests[at]


def spot_of(at, row_of, col_of, slot, rows, cols):
    return lax.rem(row_of(slot), rows) - RAD, lax.rem(col_of(slot), cols) - RAD


def pack_kernel(rows, cols, centers, live, meta, *refs):
    raw, windows, order = refs[:3], refs[3], refs[4]
    pieces, flag = dict(zip(SHIFTS, refs[5:13])), refs[13]
    bufs, piece_bufs, corner_bufs, sems, piece_sems, corner_sems = refs[14:17], refs[17:20], refs[20:23], *refs[23:26]
    slots = centers.shape[1]
    found = neighbours()

    def corner(slot):
        return lax.rem(centers[0, slot], rows) - RAD, lax.rem(centers[1, slot], cols) - RAD

    def place(slot):
        top, left = corner(slot)
        return top, left, *clamped(top, left, rows, cols)

    def copies(slot):
        _, _, row, col = place(slot)
        return [
            pltpu.make_async_copy(src.at[pl.ds(row, TALL), pl.ds(col, WIDE)], dst.at[slot], sems.at[k, slot])
            for k, (src, dst) in enumerate(zip(raw, bufs))
        ]

    def classify(slot, carry):
        inner, outer, crossing = carry
        for copy in copies(slot):
            copy.start()
        top, left = corner(slot)
        inside = is_inner(top, left, rows, cols)
        at = jnp.where(inside, inner, slots - 1 - outer)
        order[0, at] = slot
        step = inside.astype(jnp.int32)
        fresh = []
        for d, way in enumerate(MAIN):
            over = crosses(way, top, left, rows, cols) & found[way][0]
            order[2 + d, slot] = jnp.minimum(crossing[d], PIECES - 1)
            fresh.append(crossing[d] + over.astype(jnp.int32))
        return inner + step, outer + 1 - step, tuple(fresh)

    zero = jnp.int32(0)
    inner, outer, crossing = lax.fori_loop(0, live[0], classify, (zero, zero, (zero,) * 4))
    order[1, 0] = inner
    most = jnp.maximum(jnp.maximum(crossing[0], crossing[1]), jnp.maximum(crossing[2], crossing[3]))
    flag[...] = jnp.broadcast_to((most > PIECES).astype(jnp.int32), flag.shape)

    corners = []
    for n, at in enumerate(SHIFTS[4:]):
        r = pl.ds(0 if at[0] < 0 else rows - RAD, RAD)
        c = pl.ds(0 if at[1] < 0 else cols - LANES, LANES)
        corners += [
            pltpu.make_async_copy(src.at[r, c], dst.at[n], corner_sems.at[k, n])
            for k, (src, dst) in enumerate(zip(raw, corner_bufs))
        ]
    for copy in corners:
        copy.start()

    def theirs(d, slot):
        return lax.rem(meta[d, 0, slot], rows) - RAD, lax.rem(meta[d, 1, slot], cols) - RAD

    def piece_place(d, k):
        at = MAIN[d]
        top, left = theirs(d, order[6 + d, k])
        if at[1]:
            row = pl.multiple_of(jnp.clip((top + RAD) // 8 * 8 - RAD, 0, rows - TALL), 8)
            return row, 0 if at[1] < 0 else cols - LANES, top - row
        col = pl.multiple_of(jnp.clip((left + LANES) // LANES * LANES - LANES, 0, cols - WIDE), LANES)
        return 0 if at[0] < 0 else rows - RAD, col, left - col

    def piece_copies(d, k):
        row, col, _ = piece_place(d, k)
        size = (TALL, LANES) if MAIN[d][1] else (RAD, WIDE)
        return [
            pltpu.make_async_copy(
                src.at[pl.ds(row, size[0]), pl.ds(col, size[1])],
                dst.at[d, k, pl.ds(0, size[0]), pl.ds(0, size[1])],
                piece_sems.at[n, d, k],
            )
            for n, (src, dst) in enumerate(zip(raw, piece_bufs))
        ]

    counts = []
    for d, at in enumerate(MAIN):
        back = (-at[0], -at[1])

        def look(slot, count, d=d, back=back):
            top, left = theirs(d, slot)
            hit = crosses(back, top, left, rows, cols)

            @pl.when(hit & (count < PIECES))
            def _():
                order[6 + d, count] = slot
                for copy in piece_copies(d, count):
                    copy.start()

            return count + hit.astype(jnp.int32)

        limit = jnp.where(found[at][0], meta[d, 2, 0], 0)
        count = jnp.minimum(lax.fori_loop(0, limit, look, zero), PIECES)
        order[1, 1 + d] = count
        counts.append(count)

    def blank(slot, _):
        windows[0, slot] = jnp.ones((SIDE, SIDE), jnp.float32)
        windows[1, slot] = jnp.zeros((SIDE, SIDE), jnp.float32)
        return 0

    def cut(n, _):
        at = jnp.where(n < inner, n, slots - 1 - (n - inner))
        slot = order[0, at]
        for copy in copies(slot):
            copy.wait()
        top, left, row, col = place(slot)
        res, mark = turn_own(*(buf[slot] for buf in bufs), top - row, col - left)
        windows[0, at] = res
        windows[1, at] = mark
        return 0

    lax.fori_loop(inner, slots - outer, blank, 0)
    lax.fori_loop(0, live[0], cut, 0)
    for n, at in enumerate(SHIFTS[4:]):
        for k in range(3):
            corners[3 * n + k].wait()
        squeeze = pack_low if at[1] < 0 else pack_high
        res, source, target = (buf[n] for buf in corner_bufs)
        pieces[at][0] = squeeze(res)
        pieces[at][1] = squeeze(mark_of(source, target))
    for d, at in enumerate(MAIN):
        def fill(k, _, d=d, at=at):
            for copy in piece_copies(d, k):
                copy.wait()
            _, _, skip = piece_place(d, k)
            if at[1]:
                res, source, target = (buf[d, k, :, 0:LANES] for buf in piece_bufs)
                squeeze = pack_low if at[1] < 0 else pack_high
                pieces[at][0, k] = squeeze(cut_rows(res, skip))
                pieces[at][1, k] = squeeze(cut_rows(mark_of(source, target), skip))
            else:
                res, source, target = (buf[d, k, 0:RAD, :] for buf in piece_bufs)
                turn = lax.rem(2 * WIDE - skip, WIDE)
                pieces[at][0, k] = pltpu.roll(res, turn, 1)[:, :SIDE]
                pieces[at][1, k] = pltpu.roll(mark_of(source, target), turn, 1)[:, :SIDE]
            return 0

        lax.fori_loop(0, counts[d], fill, 0)


def trade_kernel(windows, flag, *refs):
    pieces = dict(zip(SHIFTS, refs[:8]))
    cur, outs, flag_out, table = refs[8], dict(zip(SHIFTS, refs[9:17])), *refs[17:19]
    halos = dict(zip(SHIFTS, refs[19:27]))
    flag_landed, send_sems, recv_sems, flag_send, flag_recv = refs[27:32]
    clear, tables, solve = solver_parts([*refs[32:], table], GROUP)
    found = neighbours()
    peers = peers_along("row")
    for at in SHIFTS:
        halos[at][...] = jnp.zeros_like(halos[at])
    hello(found, SHIFTS, peers)
    wait_for(found, SHIFTS, peers)
    copies = transfers(found, pieces, halos, send_sems, recv_sems)
    start_all(copies)
    shared = share_flag(flag, flag_landed, peers, flag_send, flag_recv)
    for copy in shared:
        copy.start()
    clear()
    tables()

    def store(b, cut, current):
        cur[b, cut, :] = current

    solve(lambda b, cut: (windows[0, b, cut, :], windows[1, b, cut, :]), store)
    for copy in shared:
        copy.wait()
    flag_out[...] = largest(flag, flag_landed, peers)
    finish_all(copies, landings(found, pieces, halos, send_sems, recv_sems))
    for at in SHIFTS:
        outs[at][...] = halos[at][...]


def unpacked(packed, dc):
    return jnp.concatenate((to_high if dc < 0 else to_low)(packed), axis=0)


def rest_kernel(rows, cols, centers, live, order, windows, inner_cur, table, *refs):
    halos, acc, outs = dict(zip(SHIFTS, refs[:8])), refs[8], dict(zip(SHIFTS, refs[9:17]))
    staged, solved = refs[17:19]
    clear, _, solve = solver_parts([*refs[19:], table], GROUP)
    solve_few = solver_parts([*refs[19:], table], PLANES)[2]
    slots = centers.shape[1]
    inner = order[1, 0]
    ready_count = jnp.minimum(inner, GROUP)
    kept = jnp.minimum(inner, GROUP + PLANES)
    acc[...] = jnp.zeros_like(acc)
    clear()
    row_id = lax.broadcasted_iota(jnp.int32, (SIDE, SIDE), 0)
    col_id = lax.broadcasted_iota(jnp.int32, (SIDE, SIDE), 1)
    blank = jnp.zeros((RAD, SIDE), jnp.float32)

    def corner(slot):
        return lax.rem(centers[0, slot], rows) - RAD, lax.rem(centers[1, slot], cols) - RAD

    def seat(n):
        return jnp.where(n < inner, n, slots - 1 - (n - inner))

    def place(n, _):
        top, left = corner(order[0, n])
        add_window(acc, inner_cur[n], top, left)
        return 0

    lax.fori_loop(0, ready_count, place, 0)

    def shifts(top, left):
        down = {-1: -top, 1: rows - top, 0: None}
        side = {-1: -left, 1: cols - left, 0: None}
        return down, side

    def ranges(at, top, left):
        at_row, at_col = row_id + top, col_id + left
        row_ok = {-1: at_row < 0, 0: (at_row >= 0) & (at_row < rows), 1: at_row >= rows}[at[0]]
        col_ok = {-1: at_col < 0, 0: (at_col >= 0) & (at_col < cols), 1: at_col >= cols}[at[1]]
        return row_ok & col_ok

    def concerns(at, top, left):
        hit = None
        for way in ((at[0], 0), (0, at[1])):
            if way != (0, 0):
                one = crosses(way, top, left, rows, cols)
                hit = one if hit is None else hit & one
        return hit

    def patch(b, slot):
        top, left = corner(slot)
        down, side = shifts(top, left)
        for d, at in enumerate(SHIFTS):
            @pl.when(concerns(at, top, left))
            def _():
                mask = ranges(at, top, left)
                for k in range(2):
                    if at[0] and at[1]:
                        tile = unpacked(halos[at][k], at[1])
                        tile = jnp.concatenate((blank, tile) if at[0] < 0 else (tile, blank), axis=0)
                    elif at[1]:
                        tile = unpacked(halos[at][k, order[2 + d, slot]], at[1])
                    else:
                        tile = halos[at][k, order[2 + d, slot]]
                        tile = jnp.concatenate((blank, tile) if at[0] < 0 else (tile, blank), axis=0)
                    if at[1]:
                        tile = pltpu.roll(tile, side[at[1]], 1)
                    if at[0]:
                        tile = pltpu.roll(tile, down[at[0]], 0)
                    staged[k, b] = jnp.where(mask, tile, staged[k, b])

        res = staged[0, b]
        staged[0, b] = jnp.where(res > 0.0, res, FAR)

    def give(b, slot):
        top, left = corner(slot)
        down, side = shifts(top, left)
        for d, at in enumerate(MAIN):
            @pl.when(concerns(at, top, left))
            def _():
                tile = jnp.where(ranges(at, top, left), solved[b], 0.0)
                if at[1]:
                    tile = pltpu.roll(tile, lax.rem(2 * SIDE - side[at[1]], SIDE), 1)
                    outs[at][order[2 + d, slot]] = (pack_high if at[1] < 0 else pack_low)(tile)
                else:
                    tile = pltpu.roll(tile, lax.rem(2 * SIDE - down[at[0]], SIDE), 0)
                    outs[at][order[2 + d, slot]] = tile[RAD:] if at[0] < 0 else tile[:RAD]

    def solve_some(first, few):
        bound, solver = (PLANES, solve_few) if few else (GROUP, solve)
        size = jnp.minimum(live[0] - first, bound)

        def ready(b, _):
            n = seat(first + jnp.minimum(b, size - 1))
            staged[0, b] = windows[0, n]
            staged[1, b] = windows[1, n]
            patch(b, order[0, n])
            return 0

        def store(b, cut, current):
            solved[b, cut, :] = current

        def done(b, _):
            slot = order[0, seat(first + b)]
            top, left = corner(slot)
            add_window(acc, solved[b], top, left)
            give(b, slot)
            return 0

        lax.fori_loop(0, bound, ready, 0)
        solver(lambda b, cut: (staged[0, b, cut, :], staged[1, b, cut, :]), store)
        lax.fori_loop(0, size, done, 0)

    left_over = live[0] - kept
    many = (left_over + GROUP - PLANES - 1) // GROUP

    def solve_group(group, _):
        solve_some(kept + group * GROUP, False)
        return 0

    lax.fori_loop(0, many, solve_group, 0)

    @pl.when(left_over > many * GROUP)
    def _():
        solve_some(kept + many * GROUP, True)

    spans = spans_of(rows, cols)
    for dr, dc in SHIFTS[4:]:
        tile = acc[spans[dr][0], spans[dc][1]]
        outs[(dr, dc)][...] = pack_high(tile) if dc < 0 else pack_low(tile)


def reply_kernel(windows, table, flag, *refs):
    pieces, outs, flag_out, cur = dict(zip(SHIFTS, refs[:8])), dict(zip(SHIFTS, refs[8:16])), *refs[16:18]
    halos = dict(zip(SHIFTS, refs[18:26]))
    flag_landed, send_sems, recv_sems, flag_send, flag_recv = refs[26:31]
    clear, _, solve = solver_parts([*refs[31:], table], PLANES)
    found = neighbours()
    peers = peers_along("col")
    for at in SHIFTS:
        halos[at][...] = jnp.zeros_like(halos[at])
    hello(found, SHIFTS, peers)
    wait_for(found, SHIFTS, peers)
    copies = transfers(found, pieces, halos, send_sems, recv_sems)
    start_all(copies)
    shared = share_flag(flag, flag_landed, peers, flag_send, flag_recv)
    for copy in shared:
        copy.start()
    clear()

    def store(b, cut, current):
        cur[b, cut, :] = current

    solve(lambda b, cut: (windows[0, GROUP + b, cut, :], windows[1, GROUP + b, cut, :]), store)
    for copy in shared:
        copy.wait()
    flag_out[...] = largest(flag, flag_landed, peers)
    finish_all(copies, landings(found, pieces, halos, send_sems, recv_sems))
    for at in SHIFTS:
        outs[at][...] = halos[at][...]


def settle_kernel(rows, cols, centers, meta, order, *refs):
    cur, halos = refs[0], dict(zip(SHIFTS, refs[1:9]))
    out, acc, out_sem = refs[10:]
    own = acc.at[pl.ds(RAD, rows), pl.ds(LANES, cols)]
    blank = jnp.zeros((RAD, SIDE), jnp.float32)
    for d, at in enumerate(MAIN):
        def add(k, _, d=d, at=at):
            slot = order[6 + d, k]
            top = lax.rem(meta[d, 0, slot], rows) - RAD
            left = lax.rem(meta[d, 1, slot], cols) - RAD
            if at[1]:
                first, second = (to_low if at[1] < 0 else to_high)(halos[at][k])
                tile = jnp.concatenate((first, second), axis=0)
                low = lanes_of(tile.shape) < RAD
                tile = jnp.where(low if at[1] < 0 else jnp.logical_not(low), tile, 0.0)
                add_window(acc, tile, top, 0 if at[1] < 0 else cols - LANES)
            else:
                tile = jnp.concatenate((halos[at][k], blank) if at[0] < 0 else (blank, halos[at][k]), axis=0)
                add_window(acc, tile, 0 if at[0] < 0 else rows - SIDE, left)
            return 0

        lax.fori_loop(0, order[1, 1 + d], add, 0)
    def place(b, _):
        slot = order[0, GROUP + b]
        top, left = lax.rem(centers[0, slot], rows) - RAD, lax.rem(centers[1, slot], cols) - RAD
        add_window(acc, cur[b], top, left)
        return 0

    lax.fori_loop(0, jnp.clip(order[1, 0] - GROUP, 0, PLANES), place, 0)
    for dr, dc in SHIFTS[4:]:
        first, second = (to_low if dc < 0 else to_high)(halos[(dr, dc)][...])
        low = lanes_of(first.shape) < RAD
        keep = low if dc < 0 else jnp.logical_not(low)
        r = RAD if dr < 0 else rows
        c = LANES if dc < 0 else cols
        for n, part in enumerate((first, second)):
            span = slice(r + RAD // 2 * n, r + RAD // 2 * n + RAD // 2), slice(c, c + LANES)
            acc[span] = acc[span] + jnp.where(keep, part, 0.0)
    store = pltpu.make_async_copy(own, out, out_sem)
    store.start()
    store.wait()


def slow_path(rows, cols, centers, live, raster):
    f32, i32 = jnp.float32, jnp.int32
    smem, vmem, hbm = (pl.BlockSpec(memory_space=m) for m in (pltpu.SMEM, pltpu.VMEM, pltpu.HBM))
    shapes = {
        at: (RAD if at[0] else rows, cols) if at[1] == 0 else ((RAD if at[0] else rows) // 2, LANES) for at in SHIFTS
    }
    pairs = [pltpu.VMEM((2, *shapes[at]), f32) for at in SHIFTS]
    strips = [pltpu.VMEM(shapes[at], f32) for at in SHIFTS]
    stage = [pltpu.VMEM((2, PLANES, SIDE, SIDE), f32), pltpu.VMEM((PLANES, SIDE, SIDE), f32)]
    kinds = (f32, i32, i32)
    frame_shapes = ((rows, LANES), (rows, LANES), (RAD, cols), (RAD, cols))
    halos = pl.pallas_call(
        functools.partial(strips_kernel, rows, cols),
        out_shape=[jax.ShapeDtypeStruct((2, *shapes[at]), f32) for at in SHIFTS],
        in_specs=[hbm] * 3,
        out_specs=[vmem] * 8,
        scratch_shapes=pairs
        + pairs
        + [pltpu.VMEM(shape, kind) for shape in frame_shapes for kind in kinds]
        + [pltpu.SemaphoreType.DMA((4, 3)), pltpu.SemaphoreType.DMA((8,)), pltpu.SemaphoreType.DMA((8,))],
        compiler_params=pltpu.CompilerParams(vmem_limit_bytes=24 << 20, collective_id=3, has_side_effects=True),
        name="strips",
    )(*raster)
    merged, *currents = pl.pallas_call(
        functools.partial(border_kernel, rows, cols),
        out_shape=[jax.ShapeDtypeStruct((rows, cols), f32)]
        + [jax.ShapeDtypeStruct(shapes[at], f32) for at in SHIFTS],
        in_specs=[smem, smem, hbm, hbm, hbm] + [vmem] * 8,
        out_specs=[hbm] + [vmem] * 8,
        scratch_shapes=[pltpu.VMEM((PLANES, TALL + SIDE, WIDE), kind) for kind in kinds]
        + [
            pltpu.SemaphoreType.DMA((3, PLANES)),
            pltpu.VMEM((2, rows + SIDE, cols + WIDE), f32),
            pltpu.VMEM((rows + SIDE, cols + WIDE), f32),
            pltpu.SemaphoreType.DMA,
        ]
        + stage
        + solver_state(PLANES),
        compiler_params=pltpu.CompilerParams(vmem_limit_bytes=42 << 20),
        name="border",
    )(centers, live, *raster, *halos)
    back = pl.pallas_call(
        return_kernel,
        out_shape=[jax.ShapeDtypeStruct(shapes[at], f32) for at in SHIFTS],
        in_specs=[vmem] * 8,
        out_specs=[vmem] * 8,
        scratch_shapes=strips + [pltpu.SemaphoreType.DMA((8,)), pltpu.SemaphoreType.DMA((8,))],
        compiler_params=pltpu.CompilerParams(vmem_limit_bytes=8 << 20, collective_id=4, has_side_effects=True),
        name="give_back",
    )(*currents)
    return pl.pallas_call(
        functools.partial(fold_kernel, rows, cols),
        out_shape=jax.ShapeDtypeStruct((rows, cols), f32),
        in_specs=[hbm] + [vmem] * 8,
        out_specs=hbm,
        scratch_shapes=[
            pltpu.VMEM((RAD, cols), f32),
            pltpu.VMEM((RAD, cols), f32),
            pltpu.VMEM((rows - SIDE, LANES), f32),
            pltpu.VMEM((rows - SIDE, LANES), f32),
            pltpu.SemaphoreType.DMA((2, 4)),
        ],
        input_output_aliases={0: 0},
        compiler_params=pltpu.CompilerParams(vmem_limit_bytes=16 << 20),
        name="fold",
    )(merged, *back)


def local(resistance, source_mask, target_mask, centers, live):
    rows, cols = resistance.shape
    raster = (resistance, source_mask, target_mask)
    centers = centers.T
    slots = centers.shape[1]
    f32, i32 = jnp.float32, jnp.int32
    smem, vmem, hbm = (pl.BlockSpec(memory_space=m) for m in (pltpu.SMEM, pltpu.VMEM, pltpu.HBM))
    dma = pltpu.SemaphoreType.DMA
    kinds = (f32, i32, i32)
    piece = {at: (RAD // 2, LANES) if at[0] and at[1] else (PIECES, RAD, LANES) for at in SHIFTS}
    twice = [(2, *piece[at]) for at in SHIFTS]
    flag_shape = jax.ShapeDtypeStruct((8, LANES), i32)
    row_peers, col_peers = lax.axis_size("row") - 1, lax.axis_size("col") - 1

    meta = pl.pallas_call(
        meta_kernel,
        out_shape=jax.ShapeDtypeStruct((len(MAIN), 8, LANES), i32),
        in_specs=[smem, smem],
        out_specs=vmem,
        scratch_shapes=[pltpu.VMEM((8, LANES), i32), pltpu.VMEM((len(MAIN), 8, LANES), i32), dma((8,)), dma((8,))],
        compiler_params=pltpu.CompilerParams(vmem_limit_bytes=1 << 20, collective_id=0, has_side_effects=True),
        name="meta",
    )(centers, live)

    windows, order, *rest = pl.pallas_call(
        functools.partial(pack_kernel, rows, cols),
        out_shape=[jax.ShapeDtypeStruct((2, slots, SIDE, SIDE), f32), jax.ShapeDtypeStruct((10, slots), i32)]
        + [jax.ShapeDtypeStruct(shape, f32) for shape in twice]
        + [flag_shape],
        in_specs=[smem, smem, smem, hbm, hbm, hbm],
        out_specs=[vmem, smem] + [vmem] * 9,
        scratch_shapes=[pltpu.VMEM((slots, TALL, WIDE), kind) for kind in kinds]
        + [pltpu.VMEM((len(MAIN), PIECES, TALL, WIDE), kind) for kind in kinds]
        + [pltpu.VMEM((4, RAD, LANES), kind) for kind in kinds]
        + [dma((3, slots)), dma((3, len(MAIN), PIECES)), dma((3, 4))],
        compiler_params=pltpu.CompilerParams(vmem_limit_bytes=40 << 20),
        name="pack",
    )(centers, live, meta, *raster)
    pieces, flag = rest[:8], rest[8]

    inner_cur, *rest = pl.pallas_call(
        trade_kernel,
        out_shape=[jax.ShapeDtypeStruct((GROUP, SIDE, SIDE), f32)]
        + [jax.ShapeDtypeStruct(shape, f32) for shape in twice]
        + [flag_shape, jax.ShapeDtypeStruct((2, PLANES * SIDE, PLANES * SIDE), jnp.bfloat16)],
        in_specs=[vmem] * 10,
        out_specs=[vmem] * 11,
        scratch_shapes=[pltpu.VMEM(shape, f32) for shape in twice]
        + [pltpu.VMEM((row_peers, 8, LANES), i32), dma((8,)), dma((8,)), dma((row_peers,)), dma((row_peers,))]
        + solver_state(GROUP, False),
        compiler_params=pltpu.CompilerParams(vmem_limit_bytes=32 << 20, collective_id=1, has_side_effects=True),
        name="trade",
    )(windows, flag, *pieces)
    halos, flag, table = rest[:8], rest[8], rest[9]

    acc_shape = jax.ShapeDtypeStruct((rows + SIDE, cols + WIDE), f32)
    acc, *pieces = pl.pallas_call(
        functools.partial(rest_kernel, rows, cols),
        out_shape=[acc_shape] + [jax.ShapeDtypeStruct(piece[at], f32) for at in SHIFTS],
        in_specs=[smem, smem, smem] + [vmem] * 11,
        out_specs=[vmem] * 9,
        scratch_shapes=[pltpu.VMEM((2, GROUP, SIDE, SIDE), f32), pltpu.VMEM((GROUP, SIDE, SIDE), f32)]
        + solver_state(GROUP, False),
        compiler_params=pltpu.CompilerParams(vmem_limit_bytes=40 << 20),
        name="rest",
    )(centers, live, order, windows, inner_cur, table, *halos)

    *halos, flag, late_cur = pl.pallas_call(
        reply_kernel,
        out_shape=[jax.ShapeDtypeStruct(piece[at], f32) for at in SHIFTS]
        + [flag_shape, jax.ShapeDtypeStruct((PLANES, SIDE, SIDE), f32)],
        in_specs=[vmem] * 11,
        out_specs=[vmem] * 10,
        scratch_shapes=[pltpu.VMEM(piece[at], f32) for at in SHIFTS]
        + [pltpu.VMEM((col_peers, 8, LANES), i32), dma((8,)), dma((8,)), dma((col_peers,)), dma((col_peers,))]
        + solver_state(PLANES, False),
        compiler_params=pltpu.CompilerParams(vmem_limit_bytes=20 << 20, collective_id=2, has_side_effects=True),
        name="reply",
    )(windows, table, flag, *pieces)

    out, _ = pl.pallas_call(
        functools.partial(settle_kernel, rows, cols),
        out_shape=[jax.ShapeDtypeStruct((rows, cols), f32), acc_shape],
        in_specs=[smem, smem, smem] + [vmem] * 10,
        out_specs=[hbm, vmem],
        scratch_shapes=[dma],
        input_output_aliases={12: 1},
        compiler_params=pltpu.CompilerParams(vmem_limit_bytes=16 << 20),
        name="settle",
    )(centers, meta, order, late_cur, *halos, acc)

    def again(carry):
        return jnp.int32(0), slow_path(rows, cols, centers, live, raster)

    return lax.while_loop(lambda carry: carry[0] > 0, again, (flag[0, 0], out))[1]


def solution(mesh):
    return jax.shard_map(
        local,
        mesh=mesh,
        in_specs=(
            P("row", "col"),
            P("row", "col"),
            P("row", "col"),
            P(("row", "col"), None),
            P(("row", "col")),
        ),
        out_specs=P("row", "col"),
        check_vma=False,
    )
```
